32 devices in a mesh: pp: 4 (over z), tp: 4 (over y, core), ep: 2 (over x).
Axes of the slice: x: 2, y: 2, z: 4, core: 2. Of those that a mesh axis runs over, the one named last changes fastest.
Arguments:
- incoming: bfloat16 [4, 1024, 2048], P('pp', ('tp', 'ep')), may hold values from -6 to 6
- expert_ids: int32 [4, 1024, 2], P('pp', ('tp', 'ep')), may hold values from 0 to 7, all different within a row; in each aligned block of 128 rows (0 to 127, 128 to 255, ..., all dimensions but the last counted through in order) at most 64 rows name the same one
- gate_scores: float32 [4, 1024, 2], P('pp', ('tp', 'ep')), may hold values from 0.05 to 1
- gate_proj: bfloat16 [8, 2048, 768], P(('tp', 'ep')), may hold values from -0.125 to 0.125
- up_proj: bfloat16 [8, 2048, 768], P(('tp', 'ep')), may hold values from -0.125 to 0.125
- down_proj: bfloat16 [8, 768, 2048], P(('tp', 'ep')), may hold values from -0.21875 to 0.21875
Outputs:
- combined: bfloat16 [4, 1024, 2048], P('pp', ('tp', 'ep'))
The draws below stay inside these ranges and needn't reach their ends.
Inputs may be any that keep to these rules, and one draw needn't show every extreme that they name: `expert_ids`: each token names 2 different experts. Among the tokens of one device of one section no expert is named more than 64 times, and in every draw some device's tokens name one expert exactly 64 times.
All inputs are finite; a program needn't handle non-finite values.
Results may differ from the reference program's by a relative error of at most 0.0045.
Values may be sent and summed in bfloat16 or wider, within the bound.
A program may use at most 64 MiB of HBM per device.

```python
import math
import jax
import jax.numpy as jnp
import numpy as np
from jax import lax

D = 2048
FF = 768
TOPK = 2
TOK_DEV = 128
EXPERTS = 8
CAP = 64
TOKENS = 1024
N_PP = 4
N_TP = 4
N_EP = 2


def steps_of(own_key, shape, pieces, low, high):
    def one(axis_at, shards_of):
        steps = jax.random.uniform(jax.random.fold_in(jax.random.fold_in(own_key, 6), axis_at), (shards_of,), jnp.float32, low / len(pieces), high / len(pieces))
        return jnp.repeat(jnp.exp(steps), shape[axis_at] // shards_of).reshape((-1,) + (1,) * (len(shape) - axis_at - 1))

    level = one(*pieces[0])
    for cut in pieces[1:]:
        level = level * one(*cut)
    return level


def deal_out(key, own, number, rows, number_of, top, most, slope):
    sequence = jax.random.permutation(key, number_of)
    heavy_load, ordinary = portions_of(number_of, rows * top, most, slope, True), portions_of(number_of, rows * top, most, slope, False)
    places = jnp.arange(number_of)

    def named(sizes, turn):
        used = int((sizes > 0).sum())
        fixed = max(1, used // 4)
        shifted = fixed + (places - fixed + turn * (used - fixed)) % max(1, number_of - fixed)
        return jnp.zeros((number_of,), jnp.int32).at[sequence[jnp.where(places < fixed, places, shifted)]].set(jnp.asarray(sizes, jnp.int32))

    sizes = jnp.where(number % 4 == 0, named(heavy_load, number // 4), named(ordinary, number - number // 4 - 1))
    mixed = jax.random.permutation(jax.random.fold_in(own, 3), number_of)
    source_of, taker = mixed[0:number_of // 2 * 2:2], mixed[1:number_of // 2 * 2:2]
    margin = jnp.minimum(sizes[source_of] - 1, most - sizes[taker]) // 2
    margin = jnp.where((source_of == sequence[0]) | (taker == sequence[0]) | (sizes[taker] == 0), 0, jnp.maximum(margin, 0))
    shifted = jax.random.randint(jax.random.fold_in(own, 4), (number_of // 2,), 0, 1 << 20) % (margin + 1)
    sizes = sizes.at[source_of].add(-shifted).at[taker].add(shifted)
    members = jnp.searchsorted(jnp.cumsum(sizes), jnp.arange(rows * top), side="right").astype(jnp.int32)
    table = members.reshape(top, rows).T
    table = table[jax.random.permutation(jax.random.fold_in(own, 1), rows)]
    turn = jax.random.randint(jax.random.fold_in(own, 2), (rows, 1), 0, top)
    return jnp.take_along_axis(table, (jnp.arange(top)[None, :] + turn) % top, axis=1)


def portions_of(amount, total, most, slope, full):
    portions = [(1 << 20) // math.isqrt(rank ** slope) + 1 for rank in range(1, amount + 1)]
    largest = most if full else min(most, max(-(-total // amount), total * portions[0] // sum(portions)))
    least = 1 if total - largest >= amount - 1 else 0
    holding, rest = [largest] + [least] * (amount - 1), total - largest - least * (amount - 1)
    while rest > 0:
        movable = [i for i in range(1, amount) if holding[i] < largest] or [i for i in range(1, amount) if holding[i] < most]
        pool, budget = sum([portions[i] for i in movable]), rest
        for i in movable:
            addition = min(most - holding[i], max(1, budget * portions[i] // pool), rest)
            holding[i] = holding[i] + addition
            rest = rest - addition
    return np.array(holding)


def noise(key, shape, deviation, most, split=(), kind=jnp.bfloat16):
    loudness = steps_of(key, shape, split, -0.22, 0.18) if split else 1.0
    values = jax.random.normal(key, shape, jnp.float32) * deviation * loudness
    return jnp.minimum(jnp.maximum(values, -most), most).astype(kind)


def setup_inputs(seed: int = 0) -> dict:
    key_list = jax.random.split(jax.random.key(seed), 7)
    incoming = noise(key_list[0], (N_PP, TOKENS, D), 1.0, 6.0, ((0, 4), (1, 8)))
    expert_ids_keys = jax.random.split(jax.random.fold_in(key_list[1], 1), N_PP * TOKENS // TOK_DEV)
    expert_ids_turns = jax.random.permutation(jax.random.fold_in(key_list[1], 3), N_PP * TOKENS // TOK_DEV)
    expert_ids = jax.vmap(lambda own, number: deal_out(jax.random.fold_in(key_list[1], 2), own, number, TOK_DEV, EXPERTS, TOPK, CAP, 2))(expert_ids_keys, expert_ids_turns).reshape((N_PP, TOKENS, TOPK))
    gate_scores = jnp.clip(jnp.exp(math.log(1.0) - 2.9957323 * jax.random.uniform(key_list[2], (N_PP, TOKENS, TOPK), jnp.float32) ** steps_of(key_list[2], (N_PP, TOKENS, TOPK), ((0, 4), (1, 8)), -0.2, 0.2)), 0.05, 1.0)
    gate_proj = noise(key_list[3], (EXPERTS, D, FF), D ** -0.5, 0.125, ((0, 8),))
    up_proj = noise(key_list[4], (EXPERTS, D, FF), D ** -0.5, 0.125, ((0, 8),))
    down_proj = noise(key_list[5], (EXPERTS, FF, D), FF ** -0.5, 0.21875, ((0, 8),))
    return {"incoming": incoming, "expert_ids": expert_ids, "gate_scores": gate_scores, "gate_proj": gate_proj, "up_proj": up_proj, "down_proj": down_proj}


def expert_apply(tokens_in, gate_mat, up_mat, down_mat):
    gate_part = jnp.dot(tokens_in, gate_mat, preferred_element_type=jnp.float32)
    upward = jnp.dot(tokens_in, up_mat, preferred_element_type=jnp.float32)
    hidden = (jax.nn.silu(gate_part) * upward).astype(jnp.bfloat16)
    return jnp.dot(hidden, down_mat, preferred_element_type=jnp.float32).astype(jnp.bfloat16)

def reference(incoming, expert_ids, gate_scores, gate_proj, up_proj, down_proj):
    arrived = jnp.roll(incoming, 1, axis=0).reshape(-1, D)
    values = arrived.astype(jnp.float32)
    normed = (values * lax.rsqrt(lax.optimization_barrier(jnp.mean(values * values, axis=1, keepdims=True)) + 1e-06)).astype(jnp.bfloat16)
    token_total = values.shape[0]
    chosen = expert_ids.reshape(-1).astype(jnp.int32)
    scores = gate_scores.reshape(token_total, TOPK)
    weights = (scores / lax.optimization_barrier(jnp.sum(scores, axis=1, keepdims=True))).reshape(-1)
    assign_total = chosen.shape[0]
    ordering = jnp.argsort(chosen, stable=True).astype(jnp.int32)
    sorted_ids = chosen[ordering]
    counts = jnp.zeros((EXPERTS,), jnp.int32).at[chosen].add(1)
    starts = jnp.cumsum(counts).astype(jnp.int32) - counts
    position = jnp.arange(assign_total, dtype=jnp.int32) - starts[sorted_ids]
    row_bound = N_PP * N_TP * N_EP * CAP
    table_tok = jnp.full((EXPERTS, row_bound), token_total, jnp.int32).at[sorted_ids, position].set(ordering // TOPK)
    table_weight = jnp.zeros((EXPERTS, row_bound), jnp.float32).at[sorted_ids, position].set(weights[ordering])
    with_blank = jnp.concatenate([normed, jnp.zeros((1, D), jnp.bfloat16)], axis=0)

    def per_expert(summed, inputs):
        gate_mat, up_mat, down_mat, tok_list, weight_list = inputs
        answered = expert_apply(with_blank[tok_list], gate_mat, up_mat, down_mat)
        return (summed.at[tok_list].add(weight_list[:, None] * answered.astype(jnp.float32)), None)
    summed, unused = lax.scan(per_expert, jnp.zeros((token_total + 1, D), jnp.float32), (gate_proj, up_proj, down_proj, table_tok, table_weight))
    combined = values + summed[:token_total]
    return combined.astype(jnp.bfloat16).reshape(incoming.shape)
```

```python
import functools

import jax
import jax.numpy as jnp
from jax import lax
from jax.experimental import pallas as pl
from jax.experimental.pallas import tpu as pltpu
from jax.sharding import PartitionSpec as P

MESH = pl.DeviceIdType.MESH
OWN, ACROSS_X, ACROSS_Y, DIAGONAL = range(4)
EARLY, LATE = range(2)


def shifted(block, axis, distance):
    devices = range(lax.axis_size(axis))
    route = [((i - distance) % len(devices), i) for i in devices]
    return lax.ppermute(block, axis, route)


def expert_apply(tokens_in, gate_mat, up_mat, down_mat):
    gate_part = jnp.dot(tokens_in, gate_mat, preferred_element_type=jnp.float32)
    upward = jnp.dot(tokens_in, up_mat, preferred_element_type=jnp.float32)
    hidden = (jax.nn.silu(gate_part) * upward).astype(jnp.bfloat16)
    return jnp.dot(hidden, down_mat, preferred_element_type=jnp.float32).astype(jnp.bfloat16)


def shards(incoming, expert_ids, gate_scores, gate_proj, up_proj, down_proj):
    arrived = shifted(incoming, "pp", 1)[0]
    tok_count, features = arrived.shape
    top_count = expert_ids.shape[2]
    expert_count = lax.axis_size("tp") * lax.axis_size("ep")
    capacity = min(tok_count, 2 * tok_count * top_count // expert_count)
    values = arrived.astype(jnp.float32)
    normed = (values * lax.rsqrt(jnp.mean(values * values, axis=1, keepdims=True) + 1e-06)).astype(
        jnp.bfloat16
    )
    chosen = expert_ids[0].reshape(-1)
    onehot = (chosen[:, None] == jnp.arange(expert_count, dtype=jnp.int32)[None, :]).astype(
        jnp.int32
    )
    before = jnp.cumsum(onehot, axis=0) - onehot
    slot_of = jnp.sum(before * onehot, axis=1)
    destination = chosen * capacity + slot_of
    owner_row = jnp.arange(chosen.shape[0], dtype=jnp.int32) // top_count
    source_row = (
        jnp.full((expert_count * capacity,), tok_count, jnp.int32).at[destination].set(owner_row)
    )
    occupied = jnp.zeros((expert_count * capacity,), jnp.int32).at[destination].set(1)
    with_blank = jnp.concatenate([normed, jnp.zeros((1, features), jnp.bfloat16)], axis=0)
    outgoing = with_blank[source_row].reshape(expert_count, capacity, features)
    occupied = occupied.reshape(expert_count, capacity)
    gate_mat, up_mat, down_mat = (gate_proj[0], up_proj[0], down_proj[0])
    received_rows = lax.all_to_all(outgoing, ("tp", "ep"), split_axis=0, concat_axis=0, tiled=True)
    flat_rows = received_rows.reshape(-1, features)
    flat_live = lax.all_to_all(
        occupied, ("tp", "ep"), split_axis=0, concat_axis=0, tiled=True
    ).reshape(-1)
    answered = expert_apply(flat_rows, gate_mat, up_mat, down_mat) * flat_live[:, None].astype(
        jnp.bfloat16
    )
    answered = answered.reshape(received_rows.shape)
    returned = lax.all_to_all(answered, ("tp", "ep"), split_axis=0, concat_axis=0, tiled=True)
    picked = returned.reshape(expert_count * capacity, features)[destination].reshape(
        tok_count, top_count, features
    )
    scores = gate_scores[0]
    weights = scores / jnp.sum(scores, axis=1, keepdims=True)
    combined = values + jnp.sum(weights[:, :, None] * picked.astype(jnp.float32), axis=1)
    return combined.astype(jnp.bfloat16)[None]


def exchange_kernel(
    sizes,
    incoming,
    ids_hbm,
    scores_hbm,
    gate_hbm,
    up_hbm,
    down_hbm,
    out_ref,
    gate_w,
    up_w,
    down_w,
    tok_early,
    tok_late,
    meta_ids,
    meta_scores,
    hidden,
    kept_early,
    kept_late,
    passed_early,
    passed_late,
    partner_early,
    partner_late,
    to_early,
    to_late,
    from_early,
    from_late,
    via_early,
    via_late,
    done_early,
    send_sem,
    recv_sem,
    load_sem,
):
    n_pp, n_tp, n_ep, top, chunks, pieces = sizes
    features, ff = gate_w.shape
    pp, tp, ep = lax.axis_index("pp"), lax.axis_index("tp"), lax.axis_index("ep")
    other_core = tp + 1 - 2 * (tp % 2)
    at_x = {"ep": (ep + 1) % n_ep}
    at_y = {"tp": (tp + 2) % n_tp}
    at_core = {"tp": other_core}
    ahead, behind = {"pp": (pp + 1) % n_pp}, {"pp": (pp + n_pp - 1) % n_pp}

    tok = (tok_early, tok_late)
    kept, passed = (kept_early, kept_late), (passed_early, passed_late)
    partner = (partner_early, partner_late)
    to, landed, via = (to_early, to_late), (from_early, from_late), (via_early, via_late)
    count = [t.shape[2] for t in tok]
    first_row = [count[LATE], 0]
    half = [n // 2 for n in count]
    part = [[pl.ds(c * (n // m), n // m) for c in range(m)] for n, m in zip(count, chunks)]

    loads = []
    for src, dst in ((gate_hbm, gate_w), (up_hbm, up_w), (down_hbm, down_w)):
        loads.append(pltpu.make_async_copy(src.at[0], dst, load_sem.at[len(loads)]))
    own_rows = pltpu.make_async_copy(
        incoming.at[0, pl.ds(first_row[EARLY], count[EARLY])], tok_early.at[OWN, 0], load_sem.at[3]
    )
    own_meta = [
        pltpu.make_async_copy(ids_hbm, meta_ids.at[0, LATE], load_sem.at[4]),
        pltpu.make_async_copy(scores_hbm, meta_scores.at[0, LATE], load_sem.at[5]),
    ]

    barrier = pltpu.get_barrier_semaphore()
    for peer in (at_x, at_y, at_core, ahead, behind):
        pl.semaphore_signal(barrier, inc=1, device_id=peer, device_id_type=MESH)
    own_rows.start()
    for copy in own_meta:
        copy.start()
    own_rows.wait()
    for copy in own_meta:
        copy.wait()
    pl.semaphore_wait(barrier, 5)

    started = []

    def link(src, dst, peer):
        i = len(started)
        copy = pltpu.make_async_remote_copy(
            src_ref=src,
            dst_ref=dst,
            send_sem=send_sem.at[i],
            recv_sem=recv_sem.at[i],
            device_id=peer,
            device_id_type=MESH,
        )
        started.append(copy)
        copy.start()
        return copy

    def block(g, role, side, c):
        return tok[g].at[role, side, part[g][c]]

    out_x, out_y, out_d, core = {}, {}, {}, {}

    def share(g, c):
        out_x[g, c] = link(block(g, OWN, 0, c), block(g, ACROSS_X, 0, c), at_x)
        out_y[g, c] = link(block(g, OWN, 0, c), block(g, ACROSS_Y, 0, c), at_y)
        core[g, OWN, c] = link(block(g, OWN, 0, c), block(g, OWN, 1, c), at_core)

    def relay(g, c):
        out_x[g, c].wait_recv()
        if c % 2 == 0:
            out_d[g, c] = link(block(g, ACROSS_X, 0, c), block(g, DIAGONAL, 0, c), at_y)
        core[g, ACROSS_X, c] = link(block(g, ACROSS_X, 0, c), block(g, ACROSS_X, 1, c), at_core)
        out_y[g, c].wait_recv()
        if c % 2 == 1:
            out_d[g, c] = link(block(g, ACROSS_Y, 0, c), block(g, DIAGONAL, 0, c), at_x)
        core[g, ACROSS_Y, c] = link(block(g, ACROSS_Y, 0, c), block(g, ACROSS_Y, 1, c), at_core)

    def relay_diagonal(g, c):
        out_d[g, c].wait_recv()
        core[g, DIAGONAL, c] = link(block(g, DIAGONAL, 0, c), block(g, DIAGONAL, 1, c), at_core)

    def meta_link(src, dst, peer):
        return [link(m.at[src], m.at[dst], peer) for m in (meta_ids, meta_scores)]

    def arrive(copies):
        for copy in copies:
            copy.wait_recv()

    mine = tp * n_ep + ep

    def weight(g, role):
        columns = []
        lane = lax.broadcasted_iota(jnp.int32, (count[g], meta_ids.shape[3]), 1)
        row = lax.broadcasted_iota(jnp.int32, (count[g], meta_ids.shape[3]), 0)
        for side in range(2):
            ids, scores = meta_ids[2 * role + side, g], meta_scores[2 * role + side, g]
            named = jnp.sum(jnp.where(ids == mine, scores, 0.0), axis=0, keepdims=True)
            share_of = named / jnp.sum(scores, axis=0, keepdims=True)
            columns.append(
                jnp.sum(jnp.where(lane == row + first_row[g], share_of, 0.0), axis=1, keepdims=True)
            )
        return columns

    swap = {}

    def expert(g, role):
        for c in range(chunks[g]):
            core[g, role, c].wait_recv()
        n = count[g]
        tokens_in = tok[g][role].reshape(2 * n, features)
        values = tokens_in.astype(jnp.float32)
        scale = lax.rsqrt(jnp.mean(values * values, axis=1, keepdims=True) + 1e-06)
        step = 256 if ff % 256 == 0 else 128
        for j in range(ff // step):
            cols = pl.ds(j * step, step)
            gate = jnp.dot(tokens_in, gate_w[:, cols], preferred_element_type=jnp.float32) * scale
            upward = jnp.dot(tokens_in, up_w[:, cols], preferred_element_type=jnp.float32) * scale
            hidden[: 2 * n, cols] = (gate / (1.0 + jnp.exp(-gate)) * upward).astype(jnp.bfloat16)
        inner = hidden[: 2 * n]
        here, there = weight(g, role)
        for j in range(features // 256):
            cols = pl.ds(j * 256, 256)
            y = jnp.dot(inner, down_w[:, cols], preferred_element_type=jnp.float32)
            y = y.astype(jnp.bfloat16).astype(jnp.float32)
            kept[g][role, :, cols] = (y[:n] * here).astype(jnp.bfloat16)
            passed[g][role, :, cols] = (y[n:] * there).astype(jnp.bfloat16)
        swap[g, role] = link(passed[g].at[role], partner[g].at[role], at_core)

    def summed(g, role, lo, hi):
        return kept[g][role, lo:hi].astype(jnp.float32) + partner[g][role, lo:hi].astype(jnp.float32)

    direct, merged, across = {}, {}, {}

    def cuts(g):
        size = half[g] // pieces
        return [(p * size, (p + 1) * size) for p in range(pieces)]

    def post(g, lane, landing, lo, hi, value, peer):
        to[g][lane, lo:hi] = value.astype(jnp.bfloat16)
        return link(to[g].at[lane, pl.ds(lo, hi - lo)], landing.at[pl.ds(lo, hi - lo)], peer)

    def send_diagonal(g):
        swap[g, DIAGONAL].wait_recv()
        for p, (lo, hi) in enumerate(cuts(g)):
            across[g, 0, p] = post(
                g, 2, via[g].at[0], lo, hi, summed(g, DIAGONAL, lo, hi), at_x
            )
            lo, hi = lo + half[g], hi + half[g]
            across[g, 1, p] = post(
                g, 2, via[g].at[0], lo, hi, summed(g, DIAGONAL, lo, hi), at_y
            )

    def send_direct(g):
        swap[g, ACROSS_X].wait_recv()
        for p, (lo, hi) in enumerate(cuts(g)):
            direct[g, 0, p] = post(g, 0, landed[g].at[0], lo, hi, summed(g, ACROSS_X, lo, hi), at_x)
        swap[g, ACROSS_Y].wait_recv()
        for p, (lo, hi) in enumerate(cuts(g)):
            lo, hi = lo + half[g], hi + half[g]
            direct[g, 1, p] = post(g, 1, landed[g].at[1], lo, hi, summed(g, ACROSS_Y, lo, hi), at_y)

    def send_merged(g):
        for p, (lo, hi) in enumerate(cuts(g)):
            across[g, 0, p].wait_recv()
            value = summed(g, ACROSS_Y, lo, hi) + via[g][0, lo:hi].astype(jnp.float32)
            merged[g, 0, p] = post(g, 1, landed[g].at[1], lo, hi, value, at_y)
            lo, hi = lo + half[g], hi + half[g]
            across[g, 1, p].wait_recv()
            value = summed(g, ACROSS_X, lo, hi) + via[g][0, lo:hi].astype(jnp.float32)
            merged[g, 1, p] = post(g, 0, landed[g].at[0], lo, hi, value, at_x)

    def finish(g):
        swap[g, OWN].wait_recv()
        for p, span in enumerate(cuts(g)):
            for k in range(2):
                lo, hi = (edge + k * half[g] for edge in span)
                value = summed(g, OWN, lo, hi) + tok[g][OWN, 0, lo:hi].astype(jnp.float32)
                direct[g, k, p].wait_recv()
                merged[g, k, p].wait_recv()
                value += landed[g][0, lo:hi].astype(jnp.float32)
                value += landed[g][1, lo:hi].astype(jnp.float32)
                value = value.astype(jnp.bfloat16)
                if g == LATE:
                    out_ref[0, lo:hi] = value
                else:
                    done_early[lo:hi] = value
                    cut = pl.ds(lo + first_row[g], hi - lo)
                    home.append(link(done_early.at[pl.ds(lo, hi - lo)], out_ref.at[0, cut], ahead))

    home = []
    hop = [
        link(incoming.at[0, part[LATE][c]], block(LATE, OWN, 0, c), ahead)
        for c in range(chunks[LATE])
    ]
    meta_early = [
        link(m.at[0, LATE], m.at[0, EARLY], behind) for m in (meta_ids, meta_scores)
    ]
    for c in range(chunks[EARLY]):
        share(EARLY, c)
    for copy in loads:
        copy.start()
    arrive(meta_early)
    meta_x = meta_link(0, 2, at_x)
    meta_y = meta_link(0, 4, at_y)
    meta_core = meta_link(0, 1, at_core)
    arrive(meta_x)
    meta_d = meta_link(2, 6, at_y)
    meta_core += meta_link(2, 3, at_core)
    arrive(meta_y)
    meta_core += meta_link(4, 5, at_core)
    for copy in loads:
        copy.wait()
    arrive(meta_core[:2])
    expert(EARLY, OWN)
    for c in range(chunks[EARLY]):
        relay(EARLY, c)
    arrive(meta_d)
    meta_core += meta_link(6, 7, at_core)
    for c in range(chunks[LATE]):
        hop[c].wait_recv()
        share(LATE, c)
    arrive(meta_core[2:])
    expert(EARLY, ACROSS_X)
    for c in range(chunks[EARLY]):
        relay_diagonal(EARLY, c)
    expert(EARLY, ACROSS_Y)
    expert(EARLY, DIAGONAL)
    for c in range(chunks[LATE]):
        relay(LATE, c)
    send_diagonal(EARLY)
    send_direct(EARLY)
    expert(LATE, OWN)
    expert(LATE, ACROSS_X)
    for c in range(chunks[LATE]):
        relay_diagonal(LATE, c)
    expert(LATE, ACROSS_Y)
    send_merged(EARLY)
    expert(LATE, DIAGONAL)
    send_diagonal(LATE)
    send_direct(LATE)
    finish(EARLY)
    send_merged(LATE)
    finish(LATE)
    arrive(home)
    for copy in started:
        copy.wait_send()


def fused(incoming, expert_ids, gate_scores, gate_proj, up_proj, down_proj):
    _, rows, features = incoming.shape
    top, ff = expert_ids.shape[2], gate_proj.shape[2]
    n_pp, n_tp, n_ep = (lax.axis_size(a) for a in ("pp", "tp", "ep"))
    early = rows // 2
    groups = (early, rows - early)
    chunks, pieces = (4, 4), 2
    hbm, vmem = pl.BlockSpec(memory_space=pl.ANY), pl.BlockSpec(memory_space=pltpu.VMEM)
    narrow = functools.partial(pltpu.VMEM, dtype=jnp.bfloat16)
    copies = 8 * sum(chunks) + 2 * 8 + 2 * 4 + 8 * 2 * pieces

    def pair(*lead):
        return [narrow((*lead, n, features)) for n in groups]

    return pl.pallas_call(
        functools.partial(exchange_kernel, (n_pp, n_tp, n_ep, top, chunks, pieces)),
        out_shape=pltpu.VMEM(incoming.shape, incoming.dtype),
        in_specs=[hbm] * 6,
        out_specs=vmem,
        scratch_shapes=[
            narrow((features, ff)),
            narrow((features, ff)),
            narrow((ff, features)),
            *pair(4, 2),
            pltpu.VMEM((8, 2, top, rows), jnp.int32),
            pltpu.VMEM((8, 2, top, rows), jnp.float32),
            narrow((2 * max(groups), ff)),
            *pair(4),
            *pair(4),
            *pair(4),
            *pair(3),
            *pair(2),
            *pair(1),
            narrow((early, features)),
            pltpu.SemaphoreType.DMA((copies,)),
            pltpu.SemaphoreType.DMA((copies,)),
            pltpu.SemaphoreType.DMA((6,)),
        ],
        compiler_params=pltpu.CompilerParams(collective_id=0, has_side_effects=True),
    )(incoming, expert_ids[0].T, gate_scores[0].T, gate_proj, up_proj, down_proj)


def solution(mesh):
    placed = (
        P("pp", ("tp", "ep"), None),
        P("pp", ("tp", "ep"), None),
        P("pp", ("tp", "ep"), None),
        P(("tp", "ep"), None, None),
        P(("tp", "ep"), None, None),
        P(("tp", "ep"), None, None),
    )
    square = mesh.shape["tp"] == 4 and mesh.shape["ep"] == 2 and mesh.shape["pp"] > 1
    return jax.shard_map(
        fused if square else shards,
        mesh=mesh,
        in_specs=placed,
        out_specs=P("pp", ("tp", "ep"), None),
        check_vma=False,
    )
```

```python
import functools

import jax
import jax.numpy as jnp
from jax import lax
from jax.experimental import pallas as pl
from jax.experimental.pallas import tpu as pltpu
from jax.sharding import PartitionSpec as P

MESH = pl.DeviceIdType.MESH
OWN, ACROSS_X, ACROSS_Y, DIAGONAL = range(4)
EARLY, LATE = range(2)


def shifted(block, axis, distance):
    devices = range(lax.axis_size(axis))
    route = [((i - distance) % len(devices), i) for i in devices]
    return lax.ppermute(block, axis, route)


def expert_apply(tokens_in, gate_mat, up_mat, down_mat):
    gate_part = jnp.dot(tokens_in, gate_mat, preferred_element_type=jnp.float32)
    upward = jnp.dot(tokens_in, up_mat, preferred_element_type=jnp.float32)
    hidden = (jax.nn.silu(gate_part) * upward).astype(jnp.bfloat16)
    return jnp.dot(hidden, down_mat, preferred_element_type=jnp.float32).astype(jnp.bfloat16)


def shards(incoming, expert_ids, gate_scores, gate_proj, up_proj, down_proj):
    arrived = shifted(incoming, "pp", 1)[0]
    tok_count, features = arrived.shape
    top_count = expert_ids.shape[2]
    expert_count = lax.axis_size("tp") * lax.axis_size("ep")
    capacity = min(tok_count, 2 * tok_count * top_count // expert_count)
    values = arrived.astype(jnp.float32)
    normed = (values * lax.rsqrt(jnp.mean(values * values, axis=1, keepdims=True) + 1e-06)).astype(
        jnp.bfloat16
    )
    chosen = expert_ids[0].reshape(-1)
    onehot = (chosen[:, None] == jnp.arange(expert_count, dtype=jnp.int32)[None, :]).astype(
        jnp.int32
    )
    before = jnp.cumsum(onehot, axis=0) - onehot
    slot_of = jnp.sum(before * onehot, axis=1)
    destination = chosen * capacity + slot_of
    owner_row = jnp.arange(chosen.shape[0], dtype=jnp.int32) // top_count
    source_row = (
        jnp.full((expert_count * capacity,), tok_count, jnp.int32).at[destination].set(owner_row)
    )
    occupied = jnp.zeros((expert_count * capacity,), jnp.int32).at[destination].set(1)
    with_blank = jnp.concatenate([normed, jnp.zeros((1, features), jnp.bfloat16)], axis=0)
    outgoing = with_blank[source_row].reshape(expert_count, capacity, features)
    occupied = occupied.reshape(expert_count, capacity)
    gate_mat, up_mat, down_mat = (gate_proj[0], up_proj[0], down_proj[0])
    received_rows = lax.all_to_all(outgoing, ("tp", "ep"), split_axis=0, concat_axis=0, tiled=True)
    flat_rows = received_rows.reshape(-1, features)
    flat_live = lax.all_to_all(
        occupied, ("tp", "ep"), split_axis=0, concat_axis=0, tiled=True
    ).reshape(-1)
    answered = expert_apply(flat_rows, gate_mat, up_mat, down_mat) * flat_live[:, None].astype(
        jnp.bfloat16
    )
    answered = answered.reshape(received_rows.shape)
    returned = lax.all_to_all(answered, ("tp", "ep"), split_axis=0, concat_axis=0, tiled=True)
    picked = returned.reshape(expert_count * capacity, features)[destination].reshape(
        tok_count, top_count, features
    )
    scores = gate_scores[0]
    weights = scores / jnp.sum(scores, axis=1, keepdims=True)
    combined = values + jnp.sum(weights[:, :, None] * picked.astype(jnp.float32), axis=1)
    return combined.astype(jnp.bfloat16)[None]


def exchange_kernel(
    sizes,
    incoming,
    ids_hbm,
    scores_hbm,
    gate_hbm,
    up_hbm,
    down_hbm,
    out_ref,
    gate_w,
    up_w,
    down_w,
    tok_early,
    tok_late,
    own_ids,
    own_scores,
    meta,
    hidden,
    kept_early,
    kept_late,
    passed_early,
    passed_late,
    partner_early,
    partner_late,
    to_early,
    to_late,
    from_early,
    from_late,
    via_early,
    via_late,
    done_early,
    send_sem,
    recv_sem,
    load_sem,
):
    n_pp, n_tp, n_ep, top, chunks, pieces = sizes
    features, ff = gate_w.shape
    pp, tp, ep = lax.axis_index("pp"), lax.axis_index("tp"), lax.axis_index("ep")
    other_core = tp + 1 - 2 * (tp % 2)
    at_x = {"ep": (ep + 1) % n_ep}
    at_y = {"tp": (tp + 2) % n_tp}
    at_core = {"tp": other_core}
    across = {"ep": (ep + 1) % n_ep, "tp": (tp + 2) % n_tp}
    ahead, behind = {"pp": (pp + 1) % n_pp}, {"pp": (pp + n_pp - 1) % n_pp}

    tok = (tok_early, tok_late)
    kept, passed = (kept_early, kept_late), (passed_early, passed_late)
    partner = (partner_early, partner_late)
    to, landed, via = (to_early, to_late), (from_early, from_late), (via_early, via_late)
    count = [t.shape[1] for t in tok]
    first_row = [count[LATE], 0]
    half = [n // 2 for n in count]
    part = [[pl.ds(c * (n // m), n // m) for c in range(m)] for n, m in zip(count, chunks)]

    loads = []
    for src, dst in ((gate_hbm, gate_w), (up_hbm, up_w), (down_hbm, down_w)):
        loads.append(pltpu.make_async_copy(src.at[0], dst, load_sem.at[len(loads)]))
    own_rows = pltpu.make_async_copy(
        incoming.at[0, pl.ds(first_row[EARLY], count[EARLY])], tok_early.at[0], load_sem.at[3]
    )
    own_meta = [
        pltpu.make_async_copy(ids_hbm, own_ids, load_sem.at[4]),
        pltpu.make_async_copy(scores_hbm, own_scores, load_sem.at[5]),
    ]

    barrier = pltpu.get_barrier_semaphore()
    for peer in (at_x, at_y, at_core, ahead, behind):
        pl.semaphore_signal(barrier, inc=1, device_id=peer, device_id_type=MESH)
    for copy in own_meta:
        copy.start()
    own_rows.start()
    for copy in own_meta:
        copy.wait()

    def meta_slot(g, source):
        return 8 * g + source

    scores = own_scores[...]
    meta[meta_slot(LATE, 0), :top] = own_ids[...].astype(jnp.float32)
    meta[meta_slot(LATE, 0), top:] = scores / jnp.sum(scores, axis=0, keepdims=True)
    own_rows.wait()
    pl.semaphore_wait(barrier, 5)

    lanes, sends = {}, {}

    def link(src, dst, peer, arrives, leaves):
        copy = pltpu.make_async_remote_copy(
            src_ref=src,
            dst_ref=dst,
            send_sem=send_sem.at[sends.setdefault(leaves, len(sends))],
            recv_sem=recv_sem.at[lanes.setdefault(arrives, len(lanes))],
            device_id=peer,
            device_id_type=MESH,
        )
        copy.start()

    def arrive(key, ref):
        sem = recv_sem.at[lanes[key]]
        pltpu.make_async_copy(ref, ref, sem).wait()

    def left(key, ref):
        sem = send_sem.at[sends[key]]
        pltpu.make_async_copy(ref, ref, sem).wait()

    def block(g, role, side, c):
        return tok[g].at[2 * role + side, part[g][c]]

    def share(g, c):
        link(block(g, OWN, 0, c), block(g, ACROSS_X, 0, c), at_x, (g, "x", c), (g, "gather"))
        link(block(g, OWN, 0, c), block(g, ACROSS_Y, 0, c), at_y, (g, "y", c), (g, "gather"))
        to_core(g, OWN, c)

    def to_core(g, role, c):
        link(block(g, role, 0, c), block(g, role, 1, c), at_core, (g, "core", role), (g, "gather"))

    def relay(g, c):
        arrive((g, "x", c), block(g, ACROSS_X, 0, c))
        if c % 2 == 0:
            link(
                block(g, ACROSS_X, 0, c), block(g, DIAGONAL, 0, c), at_y, (g, "d", c), (g, "gather")
            )
        to_core(g, ACROSS_X, c)
        arrive((g, "y", c), block(g, ACROSS_Y, 0, c))
        if c % 2 == 1:
            link(
                block(g, ACROSS_Y, 0, c), block(g, DIAGONAL, 0, c), at_x, (g, "d", c), (g, "gather")
            )
        to_core(g, ACROSS_Y, c)

    def relay_diagonal(g, c):
        arrive((g, "d", c), block(g, DIAGONAL, 0, c))
        to_core(g, DIAGONAL, c)

    def meta_link(g, src, dst, peer, name):
        src, dst = meta_slot(g, src), meta_slot(g, dst)
        link(meta.at[src], meta.at[dst], peer, (g, "meta", name), "meta")

    def meta_arrive(g, name, n=1):
        arrive((g, "meta", name), meta.at[pl.ds(0, n)])

    def meta_first(g):
        meta_link(g, 0, 2, at_x, "x")
        meta_link(g, 0, 4, at_y, "y")
        meta_link(g, 0, 1, at_core, "near")

    def meta_second(g):
        if g == LATE:
            meta_link(g, 2, 6, at_y, "d")
        else:
            meta_arrive(g, "x")
            meta_arrive(g, "y")
        meta_link(g, 2, 3, at_core, "near")
        meta_link(g, 4, 5, at_core, "near")

    def meta_third(g):
        meta_arrive(g, "d")
        meta_link(g, 6, 7, at_core, "far")

    mine = (tp * n_ep + ep).astype(jnp.float32)

    def weight(g, role):
        columns = []
        lane = lax.broadcasted_iota(jnp.int32, (count[g], meta.shape[2]), 1)
        row = lax.broadcasted_iota(jnp.int32, (count[g], meta.shape[2]), 0)
        for side in range(2):
            source = meta[meta_slot(g, 2 * role + side)]
            named = jnp.where(source[:top] == mine, source[top:], 0.0)
            named = jnp.sum(named, axis=0, keepdims=True)
            columns.append(
                jnp.sum(jnp.where(lane == row + first_row[g], named, 0.0), axis=1, keepdims=True)
            )
        return columns

    def expert(g, role):
        arrive((g, "core", role), tok[g].at[2 * role + 1])
        n = count[g]
        tokens_in = tok[g][2 * role : 2 * role + 2].reshape(2 * n, features)
        values = tokens_in.astype(jnp.float32)
        scale = lax.rsqrt(jnp.mean(values * values, axis=1, keepdims=True) + 1e-06)
        step = 256 if ff % 256 == 0 else 128
        for j in range(ff // step):
            cols = pl.ds(j * step, step)
            gate = jnp.dot(tokens_in, gate_w[:, cols], preferred_element_type=jnp.float32) * scale
            upward = jnp.dot(tokens_in, up_w[:, cols], preferred_element_type=jnp.float32) * scale
            hidden[: 2 * n, cols] = (gate / (1.0 + jnp.exp(-gate)) * upward).astype(jnp.bfloat16)
        inner = hidden[: 2 * n]
        here, there = weight(g, role)
        for j in range(features // 256):
            cols = pl.ds(j * 256, 256)
            y = jnp.dot(inner, down_w[:, cols], preferred_element_type=jnp.float32)
            y = y.astype(jnp.bfloat16).astype(jnp.float32)
            kept[g][role, :, cols] = (y[:n] * here).astype(jnp.bfloat16)
            passed[g][role, :, cols] = (y[n:] * there).astype(jnp.bfloat16)
        link(passed[g].at[role], partner[g].at[role], at_core, (g, "swap", role), (g, "return"))

    def swapped(g, role):
        arrive((g, "swap", role), partner[g].at[role])

    def summed(g, role, lo, hi):
        return kept[g][role, lo:hi].astype(jnp.float32) + partner[g][role, lo:hi].astype(jnp.float32)

    def cuts(g):
        size = half[g] // pieces
        return [(p * size, (p + 1) * size) for p in range(pieces)]

    def post(g, buffer, landing, lo, hi, value, peer, arrives):
        to[g][buffer, lo:hi] = value.astype(jnp.bfloat16)
        rows = pl.ds(lo, hi - lo)
        link(to[g].at[buffer, rows], landing.at[rows], peer, (g, *arrives), (g, "return"))

    def send_diagonal(g):
        swapped(g, DIAGONAL)
        for p, (lo, hi) in enumerate(cuts(g)):
            value = summed(g, DIAGONAL, lo, hi)
            post(g, 2, via[g], lo, hi, value, at_x, ("across", 0, p))
            lo, hi = lo + half[g], hi + half[g]
            value = summed(g, DIAGONAL, lo, hi)
            post(g, 2, via[g], lo, hi, value, at_y, ("across", 1, p))

    def send_direct(g):
        swapped(g, ACROSS_X)
        swapped(g, ACROSS_Y)
        for lo, hi in cuts(g):
            value = summed(g, ACROSS_X, lo, hi)
            post(g, 0, landed[g].at[0], lo, hi, value, at_x, ("direct", 0))
            lo, hi = lo + half[g], hi + half[g]
            value = summed(g, ACROSS_Y, lo, hi)
            post(g, 1, landed[g].at[1], lo, hi, value, at_y, ("direct", 1))

    def send_merged(g):
        for p, (lo, hi) in enumerate(cuts(g)):
            arrive((g, "across", 0, p), via[g].at[pl.ds(lo, hi - lo)])
            value = summed(g, ACROSS_Y, lo, hi) + via[g][lo:hi].astype(jnp.float32)
            post(g, 1, landed[g].at[1], lo, hi, value, at_y, ("merged", 0, p))
            lo, hi = lo + half[g], hi + half[g]
            arrive((g, "across", 1, p), via[g].at[pl.ds(lo, hi - lo)])
            value = summed(g, ACROSS_X, lo, hi) + via[g][lo:hi].astype(jnp.float32)
            post(g, 0, landed[g].at[0], lo, hi, value, at_x, ("merged", 1, p))

    def finish(g):
        swapped(g, OWN)
        for k in range(2):
            arrive((g, "direct", k), via[g].at[pl.ds(0, half[g])])
        for p, span in enumerate(cuts(g)):
            for k in range(2):
                lo, hi = (edge + k * half[g] for edge in span)
                value = summed(g, OWN, lo, hi) + tok[g][0, lo:hi].astype(jnp.float32)
                value += landed[g][k, lo:hi].astype(jnp.float32)
                arrive((g, "merged", k, p), landed[g].at[1 - k, pl.ds(lo, hi - lo)])
                value += landed[g][1 - k, lo:hi].astype(jnp.float32)
                value = value.astype(jnp.bfloat16)
                if g == LATE:
                    out_ref[0, lo:hi] = value
                else:
                    done_early[lo:hi] = value
                    cut = pl.ds(lo + first_row[g], hi - lo)
                    link(done_early.at[pl.ds(lo, hi - lo)], out_ref.at[0, cut], ahead, "home", "home")

    meta_link_back = (meta.at[meta_slot(LATE, 0)], meta.at[meta_slot(EARLY, 0)])
    link(*meta_link_back, behind, (EARLY, "meta", "own"), "meta")
    meta_first(LATE)
    for c in range(chunks[LATE]):
        link(incoming.at[0, part[LATE][c]], block(LATE, OWN, 0, c), ahead, ("hop", c), "hop")
    for c in range(chunks[EARLY] - 1):
        share(EARLY, c)
    for copy in loads:
        copy.start()
    meta_arrive(LATE, "x")
    meta_arrive(EARLY, "own")
    meta_first(EARLY)
    meta_link(EARLY, 0, 6, across, "d")
    share(EARLY, chunks[EARLY] - 1)
    meta_arrive(LATE, "y")
    meta_second(LATE)
    lag = chunks[EARLY] // 2
    for c in range(max(chunks[EARLY], chunks[LATE] + lag)):
        if c < chunks[EARLY]:
            relay(EARLY, c)
        if 0 <= c - lag < chunks[LATE]:
            arrive(("hop", c - lag), block(LATE, OWN, 0, c - lag))
            share(LATE, c - lag)
    meta_second(EARLY)
    meta_third(LATE)
    for copy in loads:
        copy.wait()
    meta_arrive(EARLY, "near", 3)
    expert(EARLY, ACROSS_X)
    meta_third(EARLY)
    expert(EARLY, ACROSS_Y)
    for c in range(chunks[EARLY]):
        relay_diagonal(EARLY, c)
    relay(LATE, 0)
    meta_arrive(EARLY, "far")
    expert(EARLY, DIAGONAL)
    for c in range(1, chunks[LATE]):
        relay(LATE, c)
    send_diagonal(EARLY)
    send_direct(EARLY)
    expert(EARLY, OWN)
    meta_arrive(LATE, "near", 3)
    meta_arrive(LATE, "far")
    expert(LATE, ACROSS_X)
    for c in range(chunks[LATE]):
        relay_diagonal(LATE, c)
    expert(LATE, ACROSS_Y)
    expert(LATE, DIAGONAL)
    send_merged(EARLY)
    send_diagonal(LATE)
    send_direct(LATE)
    expert(LATE, OWN)
    finish(EARLY)
    send_merged(LATE)
    finish(LATE)
    arrive("home", tok_early.at[0])
    left("hop", tok_late.at[0])
    left("home", tok_early.at[0])
    for g in (EARLY, LATE):
        left((g, "gather"), tok[g].at[pl.ds(0, 7)])
        left((g, "return"), tok[g].at[pl.ds(0, 7)])
    left("meta", meta.at[pl.ds(0, 15)])


def fused(incoming, expert_ids, gate_scores, gate_proj, up_proj, down_proj):
    _, rows, features = incoming.shape
    top, ff = expert_ids.shape[2], gate_proj.shape[2]
    n_pp, n_tp, n_ep = (lax.axis_size(a) for a in ("pp", "tp", "ep"))
    early = rows // 2
    groups = (early, rows - early)
    chunks, pieces = (4, 4), 2
    hbm, vmem = pl.BlockSpec(memory_space=pl.ANY), pl.BlockSpec(memory_space=pltpu.VMEM)
    narrow = functools.partial(pltpu.VMEM, dtype=jnp.bfloat16)
    arrivals = 3 * sum(chunks) + 8 + 8 + 2 * (4 * pieces + 2) + 1 + chunks[1] + 11

    def pair(*lead):
        return [narrow((*lead, n, features)) for n in groups]

    return pl.pallas_call(
        functools.partial(exchange_kernel, (n_pp, n_tp, n_ep, top, chunks, pieces)),
        out_shape=pltpu.VMEM(incoming.shape, incoming.dtype),
        in_specs=[hbm] * 6,
        out_specs=vmem,
        scratch_shapes=[
            narrow((features, ff)),
            narrow((features, ff)),
            narrow((ff, features)),
            *pair(8),
            pltpu.VMEM((top, rows), jnp.int32),
            pltpu.VMEM((top, rows), jnp.float32),
            pltpu.VMEM((16, 2 * top, rows), jnp.float32),
            narrow((2 * max(groups), ff)),
            *pair(4),
            *pair(4),
            *pair(4),
            *pair(3),
            *pair(2),
            *pair(),
            narrow((early, features)),
            pltpu.SemaphoreType.DMA((7,)),
            pltpu.SemaphoreType.DMA((arrivals,)),
            pltpu.SemaphoreType.DMA((6,)),
        ],
        compiler_params=pltpu.CompilerParams(collective_id=0, has_side_effects=True),
    )(incoming, expert_ids[0].T, gate_scores[0].T, gate_proj, up_proj, down_proj)


def solution(mesh):
    placed = (
        P("pp", ("tp", "ep"), None),
        P("pp", ("tp", "ep"), None),
        P("pp", ("tp", "ep"), None),
        P(("tp", "ep"), None, None),
        P(("tp", "ep"), None, None),
        P(("tp", "ep"), None, None),
    )
    square = mesh.shape["tp"] == 4 and mesh.shape["ep"] == 2 and mesh.shape["pp"] > 1
    return jax.shard_map(
        fused if square else shards,
        mesh=mesh,
        in_specs=placed,
        out_specs=P("pp", ("tp", "ep"), None),
        check_vma=False,
    )
```

```python
import functools

import jax
import jax.numpy as jnp
from jax import lax
from jax.experimental import pallas as pl
from jax.experimental.pallas import tpu as pltpu
from jax.sharding import PartitionSpec as P

MESH = pl.DeviceIdType.MESH
OWN, ACROSS_X, ACROSS_Y, DIAGONAL = range(4)
EARLY, LATE = range(2)


def shifted(block, axis, distance):
    devices = range(lax.axis_size(axis))
    route = [((i - distance) % len(devices), i) for i in devices]
    return lax.ppermute(block, axis, route)


def expert_apply(tokens_in, gate_mat, up_mat, down_mat):
    gate_part = jnp.dot(tokens_in, gate_mat, preferred_element_type=jnp.float32)
    upward = jnp.dot(tokens_in, up_mat, preferred_element_type=jnp.float32)
    hidden = (jax.nn.silu(gate_part) * upward).astype(jnp.bfloat16)
    return jnp.dot(hidden, down_mat, preferred_element_type=jnp.float32).astype(jnp.bfloat16)


def shards(incoming, expert_ids, gate_scores, gate_proj, up_proj, down_proj):
    arrived = shifted(incoming, "pp", 1)[0]
    tok_count, features = arrived.shape
    top_count = expert_ids.shape[2]
    expert_count = lax.axis_size("tp") * lax.axis_size("ep")
    capacity = min(tok_count, 2 * tok_count * top_count // expert_count)
    values = arrived.astype(jnp.float32)
    normed = (values * lax.rsqrt(jnp.mean(values * values, axis=1, keepdims=True) + 1e-06)).astype(
        jnp.bfloat16
    )
    chosen = expert_ids[0].reshape(-1)
    onehot = (chosen[:, None] == jnp.arange(expert_count, dtype=jnp.int32)[None, :]).astype(
        jnp.int32
    )
    before = jnp.cumsum(onehot, axis=0) - onehot
    slot_of = jnp.sum(before * onehot, axis=1)
    destination = chosen * capacity + slot_of
    owner_row = jnp.arange(chosen.shape[0], dtype=jnp.int32) // top_count
    source_row = (
        jnp.full((expert_count * capacity,), tok_count, jnp.int32).at[destination].set(owner_row)
    )
    occupied = jnp.zeros((expert_count * capacity,), jnp.int32).at[destination].set(1)
    with_blank = jnp.concatenate([normed, jnp.zeros((1, features), jnp.bfloat16)], axis=0)
    outgoing = with_blank[source_row].reshape(expert_count, capacity, features)
    occupied = occupied.reshape(expert_count, capacity)
    gate_mat, up_mat, down_mat = (gate_proj[0], up_proj[0], down_proj[0])
    received_rows = lax.all_to_all(outgoing, ("tp", "ep"), split_axis=0, concat_axis=0, tiled=True)
    flat_rows = received_rows.reshape(-1, features)
    flat_live = lax.all_to_all(
        occupied, ("tp", "ep"), split_axis=0, concat_axis=0, tiled=True
    ).reshape(-1)
    answered = expert_apply(flat_rows, gate_mat, up_mat, down_mat) * flat_live[:, None].astype(
        jnp.bfloat16
    )
    answered = answered.reshape(received_rows.shape)
    returned = lax.all_to_all(answered, ("tp", "ep"), split_axis=0, concat_axis=0, tiled=True)
    picked = returned.reshape(expert_count * capacity, features)[destination].reshape(
        tok_count, top_count, features
    )
    scores = gate_scores[0]
    weights = scores / jnp.sum(scores, axis=1, keepdims=True)
    combined = values + jnp.sum(weights[:, :, None] * picked.astype(jnp.float32), axis=1)
    return combined.astype(jnp.bfloat16)[None]


def exchange_kernel(
    sizes,
    incoming,
    ids_hbm,
    scores_hbm,
    gate_hbm,
    up_hbm,
    down_hbm,
    out_ref,
    gate_w,
    up_w,
    down_w,
    tok_early,
    tok_late,
    own_ids,
    own_scores,
    meta,
    hidden,
    kept_early,
    kept_late,
    passed_early,
    passed_late,
    partner_early,
    partner_late,
    to_early,
    to_late,
    from_early,
    from_late,
    via_early,
    via_late,
    done_early,
    send_sem,
    recv_sem,
    load_sem,
    hello,
):
    n_pp, n_tp, n_ep, top, chunks, pieces = sizes
    features, ff = gate_w.shape
    pp, tp, ep = lax.axis_index("pp"), lax.axis_index("tp"), lax.axis_index("ep")
    other_core = tp + 1 - 2 * (tp % 2)
    at_x = {"ep": (ep + 1) % n_ep}
    at_y = {"tp": (tp + 2) % n_tp}
    at_core = {"tp": other_core}
    across = {"ep": (ep + 1) % n_ep, "tp": (tp + 2) % n_tp}
    ahead, behind = {"pp": (pp + 1) % n_pp}, {"pp": (pp + n_pp - 1) % n_pp}

    tok = (tok_early, tok_late)
    kept, passed = (kept_early, kept_late), (passed_early, passed_late)
    partner = (partner_early, partner_late)
    to, landed, via = (to_early, to_late), (from_early, from_late), (via_early, via_late)
    count = [t.shape[1] for t in tok]
    first_row = [count[LATE], 0]
    half = [n // 2 for n in count]
    part = [[pl.ds(c * (n // m), n // m) for c in range(m)] for n, m in zip(count, chunks)]

    loads = []
    for src, dst in ((gate_hbm, gate_w), (up_hbm, up_w), (down_hbm, down_w)):
        loads.append(pltpu.make_async_copy(src.at[0], dst, load_sem.at[len(loads)]))
    own_rows = pltpu.make_async_copy(
        incoming.at[0, pl.ds(first_row[EARLY], count[EARLY])], tok_early.at[0], load_sem.at[3]
    )
    own_meta = [
        pltpu.make_async_copy(ids_hbm, own_ids, load_sem.at[4]),
        pltpu.make_async_copy(scores_hbm, own_scores, load_sem.at[5]),
    ]

    barrier = pltpu.get_barrier_semaphore()
    for peer in (at_x, at_y, at_core, behind):
        pl.semaphore_signal(barrier, inc=1, device_id=peer, device_id_type=MESH)
    for copy in own_meta:
        copy.start()
    own_rows.start()
    for copy in own_meta:
        copy.wait()

    def meta_slot(g, source):
        return 8 * g + source

    scores = own_scores[...]
    meta[meta_slot(LATE, 0), :top] = own_ids[...].astype(jnp.float32)
    meta[meta_slot(LATE, 0), top:] = scores / jnp.sum(scores, axis=0, keepdims=True)
    own_rows.wait()
    pl.semaphore_wait(barrier, 4)
    pl.semaphore_signal(hello, inc=1, device_id=ahead, device_id_type=MESH)

    lanes, sends = {}, {}

    def link(src, dst, peer, arrives, leaves):
        copy = pltpu.make_async_remote_copy(
            src_ref=src,
            dst_ref=dst,
            send_sem=send_sem.at[sends.setdefault(leaves, len(sends))],
            recv_sem=recv_sem.at[lanes.setdefault(arrives, len(lanes))],
            device_id=peer,
            device_id_type=MESH,
        )
        copy.start()

    def arrive(key, ref):
        sem = recv_sem.at[lanes[key]]
        pltpu.make_async_copy(ref, ref, sem).wait()

    def left(key, ref):
        sem = send_sem.at[sends[key]]
        pltpu.make_async_copy(ref, ref, sem).wait()

    def block(g, role, side, c):
        return tok[g].at[2 * role + side, part[g][c]]

    def share(g, c):
        link(block(g, OWN, 0, c), block(g, ACROSS_X, 0, c), at_x, (g, "x", c), (g, "gather"))
        link(block(g, OWN, 0, c), block(g, ACROSS_Y, 0, c), at_y, (g, "y", c), (g, "gather"))
        to_core(g, OWN, c)

    def to_core(g, role, c):
        link(block(g, role, 0, c), block(g, role, 1, c), at_core, (g, "core", role), (g, "gather"))

    def relay(g, c):
        arrive((g, "x", c), block(g, ACROSS_X, 0, c))
        if c % 2 == 0:
            link(
                block(g, ACROSS_X, 0, c), block(g, DIAGONAL, 0, c), at_y, (g, "d", c), (g, "gather")
            )
        to_core(g, ACROSS_X, c)
        arrive((g, "y", c), block(g, ACROSS_Y, 0, c))
        if c % 2 == 1:
            link(
                block(g, ACROSS_Y, 0, c), block(g, DIAGONAL, 0, c), at_x, (g, "d", c), (g, "gather")
            )
        to_core(g, ACROSS_Y, c)

    def relay_diagonal(g, c):
        arrive((g, "d", c), block(g, DIAGONAL, 0, c))
        to_core(g, DIAGONAL, c)

    def meta_link(g, src, dst, peer, name):
        src, dst = meta_slot(g, src), meta_slot(g, dst)
        link(meta.at[src], meta.at[dst], peer, (g, "meta", name), "meta")

    def meta_arrive(g, name, n=1):
        arrive((g, "meta", name), meta.at[pl.ds(0, n)])

    def meta_first(g):
        meta_link(g, 0, 2, at_x, "x")
        meta_link(g, 0, 4, at_y, "y")
        meta_link(g, 0, 1, at_core, "near")

    def meta_second(g):
        if g == LATE:
            meta_link(g, 2, 6, at_y, "d")
        else:
            meta_arrive(g, "x")
            meta_arrive(g, "y")
        meta_link(g, 2, 3, at_core, "near")
        meta_link(g, 4, 5, at_core, "near")

    def meta_third(g):
        meta_arrive(g, "d")
        meta_link(g, 6, 7, at_core, "far")

    mine = (tp * n_ep + ep).astype(jnp.float32)

    def weight(g, role):
        columns = []
        lane = lax.broadcasted_iota(jnp.int32, (count[g], meta.shape[2]), 1)
        row = lax.broadcasted_iota(jnp.int32, (count[g], meta.shape[2]), 0)
        for side in range(2):
            source = meta[meta_slot(g, 2 * role + side)]
            named = jnp.where(source[:top] == mine, source[top:], 0.0)
            named = jnp.sum(named, axis=0, keepdims=True)
            columns.append(
                jnp.sum(jnp.where(lane == row + first_row[g], named, 0.0), axis=1, keepdims=True)
            )
        return columns

    def expert(g, role, between=lambda: None):
        arrive((g, "core", role), tok[g].at[2 * role + 1])
        n = count[g]
        tokens_in = tok[g][2 * role : 2 * role + 2].reshape(2 * n, features)
        values = tokens_in.astype(jnp.float32)
        scale = lax.rsqrt(jnp.mean(values * values, axis=1, keepdims=True) + 1e-06)
        step = 256 if ff % 256 == 0 else 128
        for j in range(ff // step):
            cols = pl.ds(j * step, step)
            gate = jnp.dot(tokens_in, gate_w[:, cols], preferred_element_type=jnp.float32) * scale
            upward = jnp.dot(tokens_in, up_w[:, cols], preferred_element_type=jnp.float32) * scale
            hidden[: 2 * n, cols] = (gate / (1.0 + jnp.exp(-gate)) * upward).astype(jnp.bfloat16)
        inner = hidden[: 2 * n]
        between()
        here, there = weight(g, role)
        for j in range(features // 256):
            cols = pl.ds(j * 256, 256)
            y = jnp.dot(inner, down_w[:, cols], preferred_element_type=jnp.float32)
            y = y.astype(jnp.bfloat16).astype(jnp.float32)
            kept[g][role, :, cols] = (y[:n] * here).astype(jnp.bfloat16)
            passed[g][role, :, cols] = (y[n:] * there).astype(jnp.bfloat16)
        link(passed[g].at[role], partner[g].at[role], at_core, (g, "swap", role), (g, "return"))

    def swapped(g, role):
        arrive((g, "swap", role), partner[g].at[role])

    def summed(g, role, lo, hi):
        return kept[g][role, lo:hi].astype(jnp.float32) + partner[g][role, lo:hi].astype(jnp.float32)

    def cuts(g):
        size = half[g] // pieces
        return [(p * size, (p + 1) * size) for p in range(pieces)]

    def post(g, buffer, landing, lo, hi, value, peer, arrives):
        to[g][buffer, lo:hi] = value.astype(jnp.bfloat16)
        rows = pl.ds(lo, hi - lo)
        link(to[g].at[buffer, rows], landing.at[rows], peer, (g, *arrives), (g, "return"))

    def send_diagonal(g):
        swapped(g, DIAGONAL)
        for p, (lo, hi) in enumerate(cuts(g)):
            value = summed(g, DIAGONAL, lo, hi)
            post(g, 2, via[g], lo, hi, value, at_x, ("across", 0, p))
            lo, hi = lo + half[g], hi + half[g]
            value = summed(g, DIAGONAL, lo, hi)
            post(g, 2, via[g], lo, hi, value, at_y, ("across", 1, p))

    def send_direct(g):
        swapped(g, ACROSS_X)
        swapped(g, ACROSS_Y)
        for lo, hi in cuts(g):
            value = summed(g, ACROSS_X, lo, hi)
            post(g, 0, landed[g].at[0], lo, hi, value, at_x, ("direct",))
            lo, hi = lo + half[g], hi + half[g]
            value = summed(g, ACROSS_Y, lo, hi)
            post(g, 1, landed[g].at[1], lo, hi, value, at_y, ("direct",))

    def send_merged(g):
        for p, (lo, hi) in enumerate(cuts(g)):
            arrive((g, "across", 0, p), via[g].at[pl.ds(lo, hi - lo)])
            value = summed(g, ACROSS_Y, lo, hi) + via[g][lo:hi].astype(jnp.float32)
            post(g, 1, landed[g].at[1], lo, hi, value, at_y, ("merged", p))
            lo, hi = lo + half[g], hi + half[g]
            arrive((g, "across", 1, p), via[g].at[pl.ds(lo, hi - lo)])
            value = summed(g, ACROSS_X, lo, hi) + via[g][lo:hi].astype(jnp.float32)
            post(g, 0, landed[g].at[0], lo, hi, value, at_x, ("merged", p))

    def finish(g):
        swapped(g, OWN)
        arrive((g, "direct"), via[g])
        for p, span in enumerate(cuts(g)):
            arrive((g, "merged", p), via[g].at[pl.ds(0, 2 * (span[1] - span[0]))])
            for k in range(2):
                lo, hi = (edge + k * half[g] for edge in span)
                value = summed(g, OWN, lo, hi) + tok[g][0, lo:hi].astype(jnp.float32)
                value += landed[g][k, lo:hi].astype(jnp.float32)
                value += landed[g][1 - k, lo:hi].astype(jnp.float32)
                value = value.astype(jnp.bfloat16)
                if g == LATE:
                    out_ref[0, lo:hi] = value
                else:
                    done_early[lo:hi] = value
                    cut = pl.ds(lo + first_row[g], hi - lo)
                    link(done_early.at[pl.ds(lo, hi - lo)], out_ref.at[0, cut], ahead, "home", "home")

    def near():
        meta_second(EARLY)
        meta_arrive(EARLY, "near", 3)

    meta_first(LATE)
    for c in range(chunks[LATE]):
        link(incoming.at[0, part[LATE][c]], block(LATE, OWN, 0, c), ahead, ("hop", c), "hop")
    for c in range(chunks[EARLY] - 1):
        share(EARLY, c)
    for copy in loads:
        copy.start()
    pl.semaphore_wait(hello, 1)
    meta_link_back = (meta.at[meta_slot(LATE, 0)], meta.at[meta_slot(EARLY, 0)])
    link(*meta_link_back, behind, (EARLY, "meta", "own"), "meta")
    share(EARLY, chunks[EARLY] - 1)
    meta_arrive(LATE, "x")
    meta_arrive(LATE, "y")
    meta_second(LATE)
    lag = chunks[EARLY] // 2
    for c in range(max(chunks[EARLY], chunks[LATE] + lag)):
        if c == lag:
            meta_arrive(EARLY, "own")
            meta_first(EARLY)
            meta_link(EARLY, 0, 6, across, "d")
        if c < chunks[EARLY]:
            relay(EARLY, c)
        if 0 <= c - lag < chunks[LATE]:
            arrive(("hop", c - lag), block(LATE, OWN, 0, c - lag))
            share(LATE, c - lag)
    meta_third(LATE)
    for copy in loads:
        copy.wait()
    expert(EARLY, ACROSS_X, near)
    meta_third(EARLY)
    expert(EARLY, ACROSS_Y)
    for c in range(chunks[EARLY]):
        relay_diagonal(EARLY, c)
    relay(LATE, 0)
    meta_arrive(EARLY, "far")
    expert(EARLY, DIAGONAL)
    for c in range(1, chunks[LATE]):
        relay(LATE, c)
    send_diagonal(EARLY)
    send_direct(EARLY)
    expert(EARLY, OWN)
    meta_arrive(LATE, "near", 3)
    meta_arrive(LATE, "far")
    expert(LATE, ACROSS_X)
    for c in range(chunks[LATE]):
        relay_diagonal(LATE, c)
    expert(LATE, ACROSS_Y)
    expert(LATE, DIAGONAL)
    send_merged(EARLY)
    send_diagonal(LATE)
    send_direct(LATE)
    expert(LATE, OWN)
    finish(EARLY)
    send_merged(LATE)
    finish(LATE)
    arrive("home", tok_early.at[0])
    left("hop", tok_late.at[0])
    left("home", tok_early.at[0])
    for g in (EARLY, LATE):
        left((g, "gather"), tok[g].at[pl.ds(0, 7)])
        left((g, "return"), tok[g].at[pl.ds(0, 7)])
    left("meta", meta.at[pl.ds(0, 15)])


def fused(incoming, expert_ids, gate_scores, gate_proj, up_proj, down_proj):
    _, rows, features = incoming.shape
    top, ff = expert_ids.shape[2], gate_proj.shape[2]
    n_pp, n_tp, n_ep = (lax.axis_size(a) for a in ("pp", "tp", "ep"))
    early = rows // 2
    groups = (early, rows - early)
    chunks, pieces = (4, 4), 2
    hbm, vmem = pl.BlockSpec(memory_space=pl.ANY), pl.BlockSpec(memory_space=pltpu.VMEM)
    narrow = functools.partial(pltpu.VMEM, dtype=jnp.bfloat16)
    arrivals = 3 * sum(chunks) + 8 + 8 + 2 * (3 * pieces + 1) + 1 + chunks[1] + 11

    def pair(*lead):
        return [narrow((*lead, n, features)) for n in groups]

    return pl.pallas_call(
        functools.partial(exchange_kernel, (n_pp, n_tp, n_ep, top, chunks, pieces)),
        out_shape=pltpu.VMEM(incoming.shape, incoming.dtype),
        in_specs=[hbm] * 6,
        out_specs=vmem,
        scratch_shapes=[
            narrow((features, ff)),
            narrow((features, ff)),
            narrow((ff, features)),
            *pair(8),
            pltpu.VMEM((top, rows), jnp.int32),
            pltpu.VMEM((top, rows), jnp.float32),
            pltpu.VMEM((16, 2 * top, rows), jnp.float32),
            narrow((2 * max(groups), ff)),
            *pair(4),
            *pair(4),
            *pair(4),
            *pair(3),
            *pair(2),
            *pair(),
            narrow((early, features)),
            pltpu.SemaphoreType.DMA((7,)),
            pltpu.SemaphoreType.DMA((arrivals,)),
            pltpu.SemaphoreType.DMA((6,)),
            pltpu.SemaphoreType.REGULAR,
        ],
        compiler_params=pltpu.CompilerParams(collective_id=0, has_side_effects=True),
    )(incoming, expert_ids[0].T, gate_scores[0].T, gate_proj, up_proj, down_proj)


def solution(mesh):
    placed = (
        P("pp", ("tp", "ep"), None),
        P("pp", ("tp", "ep"), None),
        P("pp", ("tp", "ep"), None),
        P(("tp", "ep"), None, None),
        P(("tp", "ep"), None, None),
        P(("tp", "ep"), None, None),
    )
    square = mesh.shape["tp"] == 4 and mesh.shape["ep"] == 2 and mesh.shape["pp"] > 1
    return jax.shard_map(
        fused if square else shards,
        mesh=mesh,
        in_specs=placed,
        out_specs=P("pp", ("tp", "ep"), None),
        check_vma=False,
    )
```

```python
import functools

import jax
import jax.numpy as jnp
from jax import lax
from jax.experimental import pallas as pl
from jax.experimental.pallas import tpu as pltpu
from jax.sharding import PartitionSpec as P

MESH = pl.DeviceIdType.MESH
OWN, ACROSS_X, ACROSS_Y, DIAGONAL = range(4)
EARLY, LATE = range(2)


def shifted(block, axis, distance):
    devices = range(lax.axis_size(axis))
    route = [((i - distance) % len(devices), i) for i in devices]
    return lax.ppermute(block, axis, route)


def expert_apply(tokens_in, gate_mat, up_mat, down_mat):
    gate_part = jnp.dot(tokens_in, gate_mat, preferred_element_type=jnp.float32)
    upward = jnp.dot(tokens_in, up_mat, preferred_element_type=jnp.float32)
    hidden = (jax.nn.silu(gate_part) * upward).astype(jnp.bfloat16)
    return jnp.dot(hidden, down_mat, preferred_element_type=jnp.float32).astype(jnp.bfloat16)


def shards(incoming, expert_ids, gate_scores, gate_proj, up_proj, down_proj):
    arrived = shifted(incoming, "pp", 1)[0]
    tok_count, features = arrived.shape
    top_count = expert_ids.shape[2]
    expert_count = lax.axis_size("tp") * lax.axis_size("ep")
    capacity = min(tok_count, 2 * tok_count * top_count // expert_count)
    values = arrived.astype(jnp.float32)
    normed = (values * lax.rsqrt(jnp.mean(values * values, axis=1, keepdims=True) + 1e-06)).astype(
        jnp.bfloat16
    )
    chosen = expert_ids[0].reshape(-1)
    onehot = (chosen[:, None] == jnp.arange(expert_count, dtype=jnp.int32)[None, :]).astype(
        jnp.int32
    )
    before = jnp.cumsum(onehot, axis=0) - onehot
    slot_of = jnp.sum(before * onehot, axis=1)
    destination = chosen * capacity + slot_of
    owner_row = jnp.arange(chosen.shape[0], dtype=jnp.int32) // top_count
    source_row = (
        jnp.full((expert_count * capacity,), tok_count, jnp.int32).at[destination].set(owner_row)
    )
    occupied = jnp.zeros((expert_count * capacity,), jnp.int32).at[destination].set(1)
    with_blank = jnp.concatenate([normed, jnp.zeros((1, features), jnp.bfloat16)], axis=0)
    outgoing = with_blank[source_row].reshape(expert_count, capacity, features)
    occupied = occupied.reshape(expert_count, capacity)
    gate_mat, up_mat, down_mat = (gate_proj[0], up_proj[0], down_proj[0])
    received_rows = lax.all_to_all(outgoing, ("tp", "ep"), split_axis=0, concat_axis=0, tiled=True)
    flat_rows = received_rows.reshape(-1, features)
    flat_live = lax.all_to_all(
        occupied, ("tp", "ep"), split_axis=0, concat_axis=0, tiled=True
    ).reshape(-1)
    answered = expert_apply(flat_rows, gate_mat, up_mat, down_mat) * flat_live[:, None].astype(
        jnp.bfloat16
    )
    answered = answered.reshape(received_rows.shape)
    returned = lax.all_to_all(answered, ("tp", "ep"), split_axis=0, concat_axis=0, tiled=True)
    picked = returned.reshape(expert_count * capacity, features)[destination].reshape(
        tok_count, top_count, features
    )
    scores = gate_scores[0]
    weights = scores / jnp.sum(scores, axis=1, keepdims=True)
    combined = values + jnp.sum(weights[:, :, None] * picked.astype(jnp.float32), axis=1)
    return combined.astype(jnp.bfloat16)[None]


def exchange_kernel(
    sizes,
    incoming,
    ids_hbm,
    scores_hbm,
    gate_hbm,
    up_hbm,
    down_hbm,
    out_ref,
    gate_w,
    up_w,
    down_w,
    tok_early,
    tok_late,
    own_ids,
    own_scores,
    meta,
    hidden,
    kept_early,
    kept_late,
    passed_early,
    passed_late,
    partner_early,
    partner_late,
    to_early,
    to_late,
    from_early,
    from_late,
    via_early,
    via_late,
    done_early,
    send_sem,
    recv_sem,
    load_sem,
    hello,
):
    n_pp, n_tp, n_ep, top, chunks, pieces = sizes
    features, ff = gate_w.shape
    pp, tp, ep = lax.axis_index("pp"), lax.axis_index("tp"), lax.axis_index("ep")
    other_core = tp + 1 - 2 * (tp % 2)
    at_x = {"ep": (ep + 1) % n_ep}
    at_y = {"tp": (tp + 2) % n_tp}
    at_core = {"tp": other_core}
    across = {"ep": (ep + 1) % n_ep, "tp": (tp + 2) % n_tp}
    ahead, behind = {"pp": (pp + 1) % n_pp}, {"pp": (pp + n_pp - 1) % n_pp}

    tok = (tok_early, tok_late)
    kept, passed = (kept_early, kept_late), (passed_early, passed_late)
    partner = (partner_early, partner_late)
    to, landed, via = (to_early, to_late), (from_early, from_late), (via_early, via_late)
    count = [t.shape[1] for t in tok]
    first_row = [count[LATE], 0]
    half = [n // 2 for n in count]
    part = [[pl.ds(c * (n // chunks), n // chunks) for c in range(chunks)] for n in count]

    loads = []
    for src, dst in ((gate_hbm, gate_w), (up_hbm, up_w), (down_hbm, down_w)):
        loads.append(pltpu.make_async_copy(src.at[0], dst, load_sem.at[len(loads)]))
    own_rows = pltpu.make_async_copy(
        incoming.at[0, pl.ds(first_row[EARLY], count[EARLY])], tok_early.at[0], load_sem.at[3]
    )
    own_meta = [
        pltpu.make_async_copy(ids_hbm, own_ids, load_sem.at[4]),
        pltpu.make_async_copy(scores_hbm, own_scores, load_sem.at[5]),
    ]

    barrier = pltpu.get_barrier_semaphore()
    for peer in (at_x, at_y, at_core, behind):
        pl.semaphore_signal(barrier, inc=1, device_id=peer, device_id_type=MESH)
    for copy in own_meta:
        copy.start()
    own_rows.start()
    for copy in own_meta:
        copy.wait()

    def meta_slot(g, source):
        return 8 * g + source

    scores = own_scores[...]
    meta[meta_slot(LATE, 0), :top] = own_ids[...].astype(jnp.float32)
    meta[meta_slot(LATE, 0), top:] = scores / jnp.sum(scores, axis=0, keepdims=True)
    own_rows.wait()
    pl.semaphore_wait(barrier, 4)
    pl.semaphore_signal(hello, inc=1, device_id=ahead, device_id_type=MESH)

    lanes, sends = {}, {}

    def link(src, dst, peer, arrives, leaves):
        copy = pltpu.make_async_remote_copy(
            src_ref=src,
            dst_ref=dst,
            send_sem=send_sem.at[sends.setdefault(leaves, len(sends))],
            recv_sem=recv_sem.at[lanes.setdefault(arrives, len(lanes))],
            device_id=peer,
            device_id_type=MESH,
        )
        copy.start()

    def arrive(key, ref):
        sem = recv_sem.at[lanes[key]]
        pltpu.make_async_copy(ref, ref, sem).wait()

    def left(key, ref):
        sem = send_sem.at[sends[key]]
        pltpu.make_async_copy(ref, ref, sem).wait()

    def block(g, role, side, c):
        return tok[g].at[2 * role + side, part[g][c]]

    def share_x(g, c):
        link(block(g, OWN, 0, c), block(g, ACROSS_X, 0, c), at_x, (g, "x", c), (g, "gather"))
        to_core(g, OWN, c)

    def share_y(g, c):
        link(block(g, OWN, 0, c), block(g, ACROSS_Y, 0, c), at_y, (g, "y", c), (g, "gather"))

    def share(g, c):
        share_x(g, c)
        if c % 2 == 1:
            share_y(g, c)
            share_y(g, c - 1)

    def to_core(g, role, c):
        link(block(g, role, 0, c), block(g, role, 1, c), at_core, (g, "core", role), (g, "gather"))

    def relay(g, c):
        for role, name, other, i in ((ACROSS_X, "x", at_y, c), (ACROSS_Y, "y", at_x, c ^ 1)):
            arrive((g, name, i), block(g, role, 0, i))
            if c % 2 == 0:
                link(block(g, role, 0, i), block(g, DIAGONAL, 0, i), other, (g, "d", i), (g, "gather"))
            to_core(g, role, i)

    def relay_diagonal(g, c):
        arrive((g, "d", c), block(g, DIAGONAL, 0, c))
        to_core(g, DIAGONAL, c)

    def meta_link(g, src, dst, peer, name):
        src, dst = meta_slot(g, src), meta_slot(g, dst)
        link(meta.at[src], meta.at[dst], peer, (g, "meta", name), "meta")

    def meta_arrive(g, name, n=1):
        arrive((g, "meta", name), meta.at[pl.ds(0, n)])

    def meta_first(g):
        meta_link(g, 0, 2, at_x, "x")
        meta_link(g, 0, 4, at_y, "y")
        meta_link(g, 0, 1, at_core, "near")

    def meta_second(g):
        if g == LATE:
            meta_link(g, 2, 6, at_y, "d")
        else:
            meta_arrive(g, "x")
            meta_arrive(g, "y")
        meta_link(g, 2, 3, at_core, "near")
        meta_link(g, 4, 5, at_core, "near")

    def meta_third(g):
        meta_arrive(g, "d")
        meta_link(g, 6, 7, at_core, "far")

    mine = (tp * n_ep + ep).astype(jnp.float32)

    def weight(g, role):
        columns = []
        lane = lax.broadcasted_iota(jnp.int32, (count[g], meta.shape[2]), 1)
        row = lax.broadcasted_iota(jnp.int32, (count[g], meta.shape[2]), 0)
        for side in range(2):
            source = meta[meta_slot(g, 2 * role + side)]
            named = jnp.where(source[:top] == mine, source[top:], 0.0)
            named = jnp.sum(named, axis=0, keepdims=True)
            columns.append(
                jnp.sum(jnp.where(lane == row + first_row[g], named, 0.0), axis=1, keepdims=True)
            )
        return columns

    def expert(g, role):
        arrive((g, "core", role), tok[g].at[2 * role + 1])
        n = count[g]
        tokens_in = tok[g][2 * role : 2 * role + 2].reshape(2 * n, features)
        values = tokens_in.astype(jnp.float32)
        scale = lax.rsqrt(jnp.mean(values * values, axis=1, keepdims=True) + 1e-06)
        step = 256 if ff % 256 == 0 else 128
        for j in range(ff // step):
            cols = pl.ds(j * step, step)
            gate = jnp.dot(tokens_in, gate_w[:, cols], preferred_element_type=jnp.float32) * scale
            upward = jnp.dot(tokens_in, up_w[:, cols], preferred_element_type=jnp.float32) * scale
            hidden[: 2 * n, cols] = (gate / (1.0 + jnp.exp(-gate)) * upward).astype(jnp.bfloat16)
        inner = hidden[: 2 * n]
        here, there = weight(g, role)
        for j in range(features // 256):
            cols = pl.ds(j * 256, 256)
            y = jnp.dot(inner, down_w[:, cols], preferred_element_type=jnp.float32)
            y = y.astype(jnp.bfloat16).astype(jnp.float32)
            kept[g][role, :, cols] = (y[:n] * here).astype(jnp.bfloat16)
            passed[g][role, :, cols] = (y[n:] * there).astype(jnp.bfloat16)
        link(passed[g].at[role], partner[g].at[role], at_core, (g, "swap", role), (g, "return"))

    def swapped(g, role):
        arrive((g, "swap", role), partner[g].at[role])

    def summed(g, role, lo, hi):
        return kept[g][role, lo:hi].astype(jnp.float32) + partner[g][role, lo:hi].astype(jnp.float32)

    def cuts(g):
        size = half[g] // pieces
        return [(p * size, (p + 1) * size) for p in range(pieces)]

    def post(g, buffer, landing, lo, hi, value, peer, arrives):
        to[g][buffer, lo:hi] = value.astype(jnp.bfloat16)
        rows = pl.ds(lo, hi - lo)
        link(to[g].at[buffer, rows], landing.at[rows], peer, (g, *arrives), (g, "return"))

    def send_diagonal(g):
        swapped(g, DIAGONAL)
        for p, (lo, hi) in enumerate(cuts(g)):
            value = summed(g, DIAGONAL, lo, hi)
            post(g, 2, via[g], lo, hi, value, at_x, ("across", 0, p))
            lo, hi = lo + half[g], hi + half[g]
            value = summed(g, DIAGONAL, lo, hi)
            post(g, 2, via[g], lo, hi, value, at_y, ("across", 1, p))

    def send_direct(g):
        swapped(g, ACROSS_X)
        swapped(g, ACROSS_Y)
        for lo, hi in cuts(g):
            value = summed(g, ACROSS_X, lo, hi)
            post(g, 0, landed[g].at[0], lo, hi, value, at_x, ("direct",))
            lo, hi = lo + half[g], hi + half[g]
            value = summed(g, ACROSS_Y, lo, hi)
            post(g, 1, landed[g].at[1], lo, hi, value, at_y, ("direct",))

    def send_merged(g, p):
        lo, hi = cuts(g)[p]
        arrive((g, "across", 0, p), via[g].at[pl.ds(lo, hi - lo)])
        value = summed(g, ACROSS_Y, lo, hi) + via[g][lo:hi].astype(jnp.float32)
        post(g, 1, landed[g].at[1], lo, hi, value, at_y, ("merged", p))
        lo, hi = lo + half[g], hi + half[g]
        arrive((g, "across", 1, p), via[g].at[pl.ds(lo, hi - lo)])
        value = summed(g, ACROSS_X, lo, hi) + via[g][lo:hi].astype(jnp.float32)
        post(g, 0, landed[g].at[0], lo, hi, value, at_x, ("merged", p))

    def finish(g):
        swapped(g, OWN)
        arrive((g, "direct"), via[g])
        for p, span in enumerate(cuts(g)):
            arrive((g, "merged", p), via[g].at[pl.ds(0, 2 * (span[1] - span[0]))])
            for k in range(2):
                lo, hi = (edge + k * half[g] for edge in span)
                value = summed(g, OWN, lo, hi) + tok[g][0, lo:hi].astype(jnp.float32)
                value += landed[g][k, lo:hi].astype(jnp.float32)
                value += landed[g][1 - k, lo:hi].astype(jnp.float32)
                value = value.astype(jnp.bfloat16)
                if g == LATE:
                    out_ref[0, lo:hi] = value
                else:
                    done_early[lo:hi] = value
                    cut = pl.ds(lo + first_row[g], hi - lo)
                    link(done_early.at[pl.ds(lo, hi - lo)], out_ref.at[0, cut], ahead, "home", "home")

    def hopped(c):
        arrive(("hop", c), block(LATE, OWN, 0, c))
        share(LATE, c)

    meta_first(LATE)
    for c in range(chunks):
        link(incoming.at[0, part[LATE][c]], block(LATE, OWN, 0, c), ahead, ("hop", c), "hop")
    for c in range(chunks):
        share_x(EARLY, c)
        share_y(EARLY, c ^ 1)
        if c == chunks // 2:
            for copy in loads:
                copy.start()
            pl.semaphore_wait(hello, 1)
            meta_link_back = (meta.at[meta_slot(LATE, 0)], meta.at[meta_slot(EARLY, 0)])
            link(*meta_link_back, behind, (EARLY, "meta", "own"), "meta")
    meta_arrive(LATE, "x")
    meta_arrive(LATE, "y")
    meta_second(LATE)
    relay(EARLY, 0)
    relay(EARLY, 1)
    meta_arrive(EARLY, "own")
    meta_first(EARLY)
    meta_link(EARLY, 0, 6, across, "d")
    relay(EARLY, 2)
    hopped(0)
    hopped(1)
    relay(EARLY, 3)
    meta_second(EARLY)
    hopped(2)
    hopped(3)
    meta_third(LATE)
    for copy in loads:
        copy.wait()
    meta_arrive(EARLY, "near", 3)
    expert(EARLY, ACROSS_X)
    meta_third(EARLY)
    for c in range(chunks):
        relay_diagonal(EARLY, c)
    expert(EARLY, ACROSS_Y)
    relay(LATE, 0)
    meta_arrive(EARLY, "far")
    expert(EARLY, DIAGONAL)
    relay(LATE, 1)
    relay(LATE, 2)
    send_diagonal(EARLY)
    send_direct(EARLY)
    expert(EARLY, OWN)
    relay(LATE, 3)
    meta_arrive(LATE, "near", 3)
    meta_arrive(LATE, "far")
    expert(LATE, OWN)
    expert(LATE, ACROSS_X)
    for c in range(chunks):
        relay_diagonal(LATE, c)
    expert(LATE, ACROSS_Y)
    send_merged(EARLY, 0)
    expert(LATE, DIAGONAL)
    send_merged(EARLY, 1)
    send_diagonal(LATE)
    send_direct(LATE)
    finish(EARLY)
    send_merged(LATE, 0)
    send_merged(LATE, 1)
    finish(LATE)
    arrive("home", tok_early.at[0])
    left("hop", tok_late.at[0])
    left("home", tok_early.at[0])
    for g in (EARLY, LATE):
        left((g, "gather"), tok[g].at[pl.ds(0, 7)])
        left((g, "return"), tok[g].at[pl.ds(0, 7)])
    left("meta", meta.at[pl.ds(0, 15)])


def fused(incoming, expert_ids, gate_scores, gate_proj, up_proj, down_proj):
    _, rows, features = incoming.shape
    top, ff = expert_ids.shape[2], gate_proj.shape[2]
    n_pp, n_tp, n_ep = (lax.axis_size(a) for a in ("pp", "tp", "ep"))
    early = rows // 2
    groups = (early, rows - early)
    chunks, pieces = 4, 2
    hbm, vmem = pl.BlockSpec(memory_space=pl.ANY), pl.BlockSpec(memory_space=pltpu.VMEM)
    narrow = functools.partial(pltpu.VMEM, dtype=jnp.bfloat16)
    arrivals = 7 * chunks + 8 + 8 + 2 * (3 * pieces + 1) + 1 + 11

    def pair(*lead):
        return [narrow((*lead, n, features)) for n in groups]

    return pl.pallas_call(
        functools.partial(exchange_kernel, (n_pp, n_tp, n_ep, top, chunks, pieces)),
        out_shape=pltpu.VMEM(incoming.shape, incoming.dtype),
        in_specs=[hbm] * 6,
        out_specs=vmem,
        scratch_shapes=[
            narrow((features, ff)),
            narrow((features, ff)),
            narrow((ff, features)),
            *pair(8),
            pltpu.VMEM((top, rows), jnp.int32),
            pltpu.VMEM((top, rows), jnp.float32),
            pltpu.VMEM((16, 2 * top, rows), jnp.float32),
            narrow((2 * max(groups), ff)),
            *pair(4),
            *pair(4),
            *pair(4),
            *pair(3),
            *pair(2),
            *pair(),
            narrow((early, features)),
            pltpu.SemaphoreType.DMA((7,)),
            pltpu.SemaphoreType.DMA((arrivals,)),
            pltpu.SemaphoreType.DMA((6,)),
            pltpu.SemaphoreType.REGULAR,
        ],
        compiler_params=pltpu.CompilerParams(collective_id=0, has_side_effects=True),
    )(incoming, expert_ids[0].T, gate_scores[0].T, gate_proj, up_proj, down_proj)


def solution(mesh):
    placed = (
        P("pp", ("tp", "ep"), None),
        P("pp", ("tp", "ep"), None),
        P("pp", ("tp", "ep"), None),
        P(("tp", "ep"), None, None),
        P(("tp", "ep"), None, None),
        P(("tp", "ep"), None, None),
    )
    square = mesh.shape["tp"] == 4 and mesh.shape["ep"] == 2 and mesh.shape["pp"] > 1
    return jax.shard_map(
        fused if square else shards,
        mesh=mesh,
        in_specs=placed,
        out_specs=P("pp", ("tp", "ep"), None),
        check_vma=False,
    )
```

```python
import functools

import jax
import jax.numpy as jnp
from jax import lax
from jax.experimental import pallas as pl
from jax.experimental.pallas import tpu as pltpu
from jax.sharding import PartitionSpec as P

MESH = pl.DeviceIdType.MESH
OWN, ACROSS_X, ACROSS_Y, DIAGONAL = range(4)
EARLY, LATE = range(2)


def shifted(block, axis, distance):
    devices = range(lax.axis_size(axis))
    route = [((i - distance) % len(devices), i) for i in devices]
    return lax.ppermute(block, axis, route)


def expert_apply(tokens_in, gate_mat, up_mat, down_mat):
    gate_part = jnp.dot(tokens_in, gate_mat, preferred_element_type=jnp.float32)
    upward = jnp.dot(tokens_in, up_mat, preferred_element_type=jnp.float32)
    hidden = (jax.nn.silu(gate_part) * upward).astype(jnp.bfloat16)
    return jnp.dot(hidden, down_mat, preferred_element_type=jnp.float32).astype(jnp.bfloat16)


def shards(incoming, expert_ids, gate_scores, gate_proj, up_proj, down_proj):
    arrived = shifted(incoming, "pp", 1)[0]
    tok_count, features = arrived.shape
    top_count = expert_ids.shape[2]
    expert_count = lax.axis_size("tp") * lax.axis_size("ep")
    capacity = min(tok_count, 2 * tok_count * top_count // expert_count)
    values = arrived.astype(jnp.float32)
    normed = (values * lax.rsqrt(jnp.mean(values * values, axis=1, keepdims=True) + 1e-06)).astype(
        jnp.bfloat16
    )
    chosen = expert_ids[0].reshape(-1)
    onehot = (chosen[:, None] == jnp.arange(expert_count, dtype=jnp.int32)[None, :]).astype(
        jnp.int32
    )
    before = jnp.cumsum(onehot, axis=0) - onehot
    slot_of = jnp.sum(before * onehot, axis=1)
    destination = chosen * capacity + slot_of
    owner_row = jnp.arange(chosen.shape[0], dtype=jnp.int32) // top_count
    source_row = (
        jnp.full((expert_count * capacity,), tok_count, jnp.int32).at[destination].set(owner_row)
    )
    occupied = jnp.zeros((expert_count * capacity,), jnp.int32).at[destination].set(1)
    with_blank = jnp.concatenate([normed, jnp.zeros((1, features), jnp.bfloat16)], axis=0)
    outgoing = with_blank[source_row].reshape(expert_count, capacity, features)
    occupied = occupied.reshape(expert_count, capacity)
    gate_mat, up_mat, down_mat = (gate_proj[0], up_proj[0], down_proj[0])
    received_rows = lax.all_to_all(outgoing, ("tp", "ep"), split_axis=0, concat_axis=0, tiled=True)
    flat_rows = received_rows.reshape(-1, features)
    flat_live = lax.all_to_all(
        occupied, ("tp", "ep"), split_axis=0, concat_axis=0, tiled=True
    ).reshape(-1)
    answered = expert_apply(flat_rows, gate_mat, up_mat, down_mat) * flat_live[:, None].astype(
        jnp.bfloat16
    )
    answered = answered.reshape(received_rows.shape)
    returned = lax.all_to_all(answered, ("tp", "ep"), split_axis=0, concat_axis=0, tiled=True)
    picked = returned.reshape(expert_count * capacity, features)[destination].reshape(
        tok_count, top_count, features
    )
    scores = gate_scores[0]
    weights = scores / jnp.sum(scores, axis=1, keepdims=True)
    combined = values + jnp.sum(weights[:, :, None] * picked.astype(jnp.float32), axis=1)
    return combined.astype(jnp.bfloat16)[None]


def exchange_kernel(
    sizes,
    incoming,
    ids_hbm,
    scores_hbm,
    gate_hbm,
    up_hbm,
    down_hbm,
    out_ref,
    gate_w,
    up_w,
    down_w,
    tok_early,
    tok_late,
    own_ids,
    own_scores,
    meta,
    hidden,
    kept_early,
    kept_late,
    passed_early,
    passed_late,
    partner_early,
    partner_late,
    to_early,
    to_late,
    from_early,
    from_late,
    via_early,
    via_late,
    done_early,
    send_sem,
    recv_sem,
    load_sem,
    hello,
):
    n_pp, n_tp, n_ep, top, chunks, pieces = sizes
    features, ff = gate_w.shape
    pp, tp, ep = lax.axis_index("pp"), lax.axis_index("tp"), lax.axis_index("ep")
    other_core = tp + 1 - 2 * (tp % 2)
    at_x = {"ep": (ep + 1) % n_ep}
    at_y = {"tp": (tp + 2) % n_tp}
    at_core = {"tp": other_core}
    across = {"ep": (ep + 1) % n_ep, "tp": (tp + 2) % n_tp}
    ahead, behind = {"pp": (pp + 1) % n_pp}, {"pp": (pp + n_pp - 1) % n_pp}

    tok = (tok_early, tok_late)
    kept, passed = (kept_early, kept_late), (passed_early, passed_late)
    partner = (partner_early, partner_late)
    to, landed, via = (to_early, to_late), (from_early, from_late), (via_early, via_late)
    count = [t.shape[1] for t in tok]
    first_row = [count[LATE], 0]
    half = [n // 2 for n in count]
    part = [[pl.ds(c * (n // chunks), n // chunks) for c in range(chunks)] for n in count]

    loads = []
    for src, dst in ((gate_hbm, gate_w), (up_hbm, up_w), (down_hbm, down_w)):
        loads.append(pltpu.make_async_copy(src.at[0], dst, load_sem.at[len(loads)]))
    own_rows = pltpu.make_async_copy(
        incoming.at[0, pl.ds(first_row[EARLY], count[EARLY])], tok_early.at[0], load_sem.at[3]
    )
    own_meta = [
        pltpu.make_async_copy(ids_hbm, own_ids, load_sem.at[4]),
        pltpu.make_async_copy(scores_hbm, own_scores, load_sem.at[5]),
    ]

    barrier = pltpu.get_barrier_semaphore()
    for peer in (at_x, at_y, at_core, behind):
        pl.semaphore_signal(barrier, inc=1, device_id=peer, device_id_type=MESH)
    for copy in own_meta:
        copy.start()
    own_rows.start()
    for copy in own_meta:
        copy.wait()

    def meta_slot(g, source):
        return 8 * g + source

    scores = own_scores[...]
    meta[meta_slot(LATE, 0), :top] = own_ids[...].astype(jnp.float32)
    meta[meta_slot(LATE, 0), top:] = scores / jnp.sum(scores, axis=0, keepdims=True)
    own_rows.wait()
    pl.semaphore_wait(barrier, 4)
    pl.semaphore_signal(hello, inc=1, device_id=ahead, device_id_type=MESH)

    lanes, sends = {}, {}

    def link(src, dst, peer, arrives, leaves):
        copy = pltpu.make_async_remote_copy(
            src_ref=src,
            dst_ref=dst,
            send_sem=send_sem.at[sends.setdefault(leaves, len(sends))],
            recv_sem=recv_sem.at[lanes.setdefault(arrives, len(lanes))],
            device_id=peer,
            device_id_type=MESH,
        )
        copy.start()

    def arrive(key, ref):
        sem = recv_sem.at[lanes[key]]
        pltpu.make_async_copy(ref, ref, sem).wait()

    def left(key, ref):
        sem = send_sem.at[sends[key]]
        pltpu.make_async_copy(ref, ref, sem).wait()

    def block(g, role, side, c):
        return tok[g].at[2 * role + side, part[g][c]]

    def share_x(g, c):
        link(block(g, OWN, 0, c), block(g, ACROSS_X, 0, c), at_x, (g, "plane", c), (g, "gather"))
        to_core(g, OWN, c)

    def share_y(g, c):
        link(block(g, OWN, 0, c), block(g, ACROSS_Y, 0, c), at_y, (g, "plane", c ^ 1), (g, "gather"))

    def share(g, c):
        share_x(g, c)
        if c % 2 == 1:
            share_y(g, c)
            share_y(g, c - 1)

    def to_core(g, role, c):
        link(block(g, role, 0, c), block(g, role, 1, c), at_core, (g, "core", role), (g, "gather"))

    def relay(g, c):
        arrive((g, "plane", c), tok[g].at[0, pl.ds(0, 2 * (count[g] // chunks))])
        for role, other, i in ((ACROSS_X, at_y, c), (ACROSS_Y, at_x, c ^ 1)):
            if c % 2 == 0:
                link(block(g, role, 0, i), block(g, DIAGONAL, 0, i), other, (g, "d"), (g, "gather"))
            to_core(g, role, i)

    def relay_diagonal(g):
        there, here = (tok[g].at[2 * DIAGONAL + side] for side in (1, 0))
        arrive((g, "d"), here)
        link(here, there, at_core, (g, "core", DIAGONAL), (g, "gather"))

    def meta_link(g, src, dst, peer, name):
        src, dst = meta_slot(g, src), meta_slot(g, dst)
        link(meta.at[src], meta.at[dst], peer, (g, "meta", name), "meta")

    def meta_arrive(g, name, n=1):
        arrive((g, "meta", name), meta.at[pl.ds(0, n)])

    def meta_first(g):
        meta_link(g, 0, 2, at_x, "plane")
        meta_link(g, 0, 4, at_y, "plane")
        meta_link(g, 0, 1, at_core, "near")

    def meta_second(g):
        if g == LATE:
            meta_link(g, 2, 6, at_y, "d")
        else:
            meta_arrive(g, "plane", 2)
        meta_link(g, 2, 3, at_core, "near")
        meta_link(g, 4, 5, at_core, "near")

    def meta_third(g):
        meta_arrive(g, "d")
        meta_link(g, 6, 7, at_core, "far" if g == EARLY else "near")

    mine = (tp * n_ep + ep).astype(jnp.float32)

    def weight(g, role):
        columns = []
        lane = lax.broadcasted_iota(jnp.int32, (count[g], meta.shape[2]), 1)
        row = lax.broadcasted_iota(jnp.int32, (count[g], meta.shape[2]), 0)
        for side in range(2):
            source = meta[meta_slot(g, 2 * role + side)]
            named = jnp.where(source[:top] == mine, source[top:], 0.0)
            named = jnp.sum(named, axis=0, keepdims=True)
            columns.append(
                jnp.sum(jnp.where(lane == row + first_row[g], named, 0.0), axis=1, keepdims=True)
            )
        return columns

    def expert(g, role):
        arrive((g, "core", role), tok[g].at[2 * role + 1])
        n = count[g]
        tokens_in = tok[g][2 * role : 2 * role + 2].reshape(2 * n, features)
        values = tokens_in.astype(jnp.float32)
        scale = lax.rsqrt(jnp.mean(values * values, axis=1, keepdims=True) + 1e-06)
        step = 256 if ff % 256 == 0 else 128
        for j in range(ff // step):
            cols = pl.ds(j * step, step)
            gate = jnp.dot(tokens_in, gate_w[:, cols], preferred_element_type=jnp.float32) * scale
            upward = jnp.dot(tokens_in, up_w[:, cols], preferred_element_type=jnp.float32) * scale
            hidden[: 2 * n, cols] = (gate / (1.0 + jnp.exp(-gate)) * upward).astype(jnp.bfloat16)
        inner = hidden[: 2 * n]
        here, there = weight(g, role)
        for j in range(features // 256):
            cols = pl.ds(j * 256, 256)
            y = jnp.dot(inner, down_w[:, cols], preferred_element_type=jnp.float32)
            y = y.astype(jnp.bfloat16).astype(jnp.float32)
            kept[g][role, :, cols] = (y[:n] * here).astype(jnp.bfloat16)
            passed[g][role, :, cols] = (y[n:] * there).astype(jnp.bfloat16)
        link(passed[g].at[role], partner[g].at[role], at_core, (g, "swap", role), (g, "return"))

    def swapped(g, role):
        arrive((g, "swap", role), partner[g].at[role])

    def summed(g, role, lo, hi):
        return kept[g][role, lo:hi].astype(jnp.float32) + partner[g][role, lo:hi].astype(jnp.float32)

    def cuts(g):
        size = half[g] // pieces
        return [(p * size, (p + 1) * size) for p in range(pieces)]

    def post(g, buffer, landing, lo, hi, value, peer, arrives):
        to[g][buffer, lo:hi] = value.astype(jnp.bfloat16)
        rows = pl.ds(lo, hi - lo)
        link(to[g].at[buffer, rows], landing.at[rows], peer, (g, *arrives), (g, "return"))

    def send_diagonal(g):
        swapped(g, DIAGONAL)
        for p, (lo, hi) in enumerate(cuts(g)):
            value = summed(g, DIAGONAL, lo, hi)
            post(g, 2, via[g], lo, hi, value, at_x, ("across", p))
            lo, hi = lo + half[g], hi + half[g]
            value = summed(g, DIAGONAL, lo, hi)
            post(g, 2, via[g], lo, hi, value, at_y, ("across", p))

    def send_direct(g):
        swapped(g, ACROSS_X)
        swapped(g, ACROSS_Y)
        for lo, hi in cuts(g):
            value = summed(g, ACROSS_X, lo, hi)
            post(g, 0, landed[g].at[0], lo, hi, value, at_x, ("direct",))
            lo, hi = lo + half[g], hi + half[g]
            value = summed(g, ACROSS_Y, lo, hi)
            post(g, 1, landed[g].at[1], lo, hi, value, at_y, ("direct",))

    def send_merged(g, p):
        lo, hi = cuts(g)[p]
        arrive((g, "across", p), via[g].at[pl.ds(0, 2 * (hi - lo))])
        value = summed(g, ACROSS_Y, lo, hi) + via[g][lo:hi].astype(jnp.float32)
        post(g, 1, landed[g].at[1], lo, hi, value, at_y, ("merged", p))
        lo, hi = lo + half[g], hi + half[g]
        value = summed(g, ACROSS_X, lo, hi) + via[g][lo:hi].astype(jnp.float32)
        post(g, 0, landed[g].at[0], lo, hi, value, at_x, ("merged", p))

    def finish(g):
        swapped(g, OWN)
        arrive((g, "direct"), via[g])
        for p, span in enumerate(cuts(g)):
            arrive((g, "merged", p), via[g].at[pl.ds(0, 2 * (span[1] - span[0]))])
            for k in range(2):
                lo, hi = (edge + k * half[g] for edge in span)
                value = summed(g, OWN, lo, hi) + tok[g][0, lo:hi].astype(jnp.float32)
                value += landed[g][k, lo:hi].astype(jnp.float32)
                value += landed[g][1 - k, lo:hi].astype(jnp.float32)
                value = value.astype(jnp.bfloat16)
                if g == LATE:
                    out_ref[0, lo:hi] = value
                else:
                    done_early[lo:hi] = value
                    cut = pl.ds(lo + first_row[g], hi - lo)
                    link(done_early.at[pl.ds(lo, hi - lo)], out_ref.at[0, cut], ahead, "home", "home")

    def hopped(c):
        arrive(("hop", c), block(LATE, OWN, 0, c))
        share(LATE, c)

    meta_first(LATE)
    for c in range(chunks):
        link(incoming.at[0, part[LATE][c]], block(LATE, OWN, 0, c), ahead, ("hop", c), "hop")
    for c in range(chunks):
        share_x(EARLY, c)
        share_y(EARLY, c ^ 1)
        if c == chunks // 2:
            for copy in loads:
                copy.start()
            pl.semaphore_wait(hello, 1)
            meta_link_back = (meta.at[meta_slot(LATE, 0)], meta.at[meta_slot(EARLY, 0)])
            link(*meta_link_back, behind, (EARLY, "meta", "own"), "meta")
    meta_arrive(LATE, "plane", 2)
    meta_second(LATE)
    relay(EARLY, 0)
    relay(EARLY, 1)
    meta_arrive(EARLY, "own")
    meta_first(EARLY)
    meta_link(EARLY, 0, 6, across, "d")
    relay(EARLY, 2)
    hopped(0)
    hopped(1)
    relay(EARLY, 3)
    meta_second(EARLY)
    hopped(2)
    hopped(3)
    meta_third(LATE)
    for copy in loads:
        copy.wait()
    meta_arrive(EARLY, "near", 3)
    expert(EARLY, ACROSS_X)
    meta_third(EARLY)
    relay_diagonal(EARLY)
    expert(EARLY, ACROSS_Y)
    relay(LATE, 0)
    meta_arrive(EARLY, "far")
    expert(EARLY, DIAGONAL)
    relay(LATE, 1)
    relay(LATE, 2)
    send_diagonal(EARLY)
    send_direct(EARLY)
    relay(LATE, 3)
    expert(EARLY, OWN)
    meta_arrive(LATE, "near", 4)
    expert(LATE, ACROSS_X)
    relay_diagonal(LATE)
    expert(LATE, ACROSS_Y)
    send_merged(EARLY, 0)
    expert(LATE, DIAGONAL)
    send_merged(EARLY, 1)
    send_diagonal(LATE)
    send_direct(LATE)
    expert(LATE, OWN)
    finish(EARLY)
    send_merged(LATE, 0)
    send_merged(LATE, 1)
    finish(LATE)
    arrive("home", tok_early.at[0])
    left("hop", tok_late.at[0])
    left("home", tok_early.at[0])
    for g in (EARLY, LATE):
        left((g, "gather"), tok[g].at[pl.ds(0, 7)])
        left((g, "return"), tok[g].at[pl.ds(0, 7)])
    left("meta", meta.at[pl.ds(0, 15)])


def fused(incoming, expert_ids, gate_scores, gate_proj, up_proj, down_proj):
    _, rows, features = incoming.shape
    top, ff = expert_ids.shape[2], gate_proj.shape[2]
    n_pp, n_tp, n_ep = (lax.axis_size(a) for a in ("pp", "tp", "ep"))
    early = rows // 2
    groups = (early, rows - early)
    chunks, pieces = 4, 2
    hbm, vmem = pl.BlockSpec(memory_space=pl.ANY), pl.BlockSpec(memory_space=pltpu.VMEM)
    narrow = functools.partial(pltpu.VMEM, dtype=jnp.bfloat16)
    arrivals = 3 * chunks + 2 * (1 + 4 + 4 + 2 * pieces + 1) + 1 + 8

    def pair(*lead):
        return [narrow((*lead, n, features)) for n in groups]

    return pl.pallas_call(
        functools.partial(exchange_kernel, (n_pp, n_tp, n_ep, top, chunks, pieces)),
        out_shape=pltpu.VMEM(incoming.shape, incoming.dtype),
        in_specs=[hbm] * 6,
        out_specs=vmem,
        scratch_shapes=[
            narrow((features, ff)),
            narrow((features, ff)),
            narrow((ff, features)),
            *pair(8),
            pltpu.VMEM((top, rows), jnp.int32),
            pltpu.VMEM((top, rows), jnp.float32),
            pltpu.VMEM((16, 2 * top, rows), jnp.float32),
            narrow((2 * max(groups), ff)),
            *pair(4),
            *pair(4),
            *pair(4),
            *pair(3),
            *pair(2),
            *pair(),
            narrow((early, features)),
            pltpu.SemaphoreType.DMA((7,)),
            pltpu.SemaphoreType.DMA((arrivals,)),
            pltpu.SemaphoreType.DMA((6,)),
            pltpu.SemaphoreType.REGULAR,
        ],
        compiler_params=pltpu.CompilerParams(collective_id=0, has_side_effects=True),
    )(incoming, expert_ids[0].T, gate_scores[0].T, gate_proj, up_proj, down_proj)


def solution(mesh):
    placed = (
        P("pp", ("tp", "ep"), None),
        P("pp", ("tp", "ep"), None),
        P("pp", ("tp", "ep"), None),
        P(("tp", "ep"), None, None),
        P(("tp", "ep"), None, None),
        P(("tp", "ep"), None, None),
    )
    square = mesh.shape["tp"] == 4 and mesh.shape["ep"] == 2 and mesh.shape["pp"] > 1
    return jax.shard_map(
        fused if square else shards,
        mesh=mesh,
        in_specs=placed,
        out_specs=P("pp", ("tp", "ep"), None),
        check_vma=False,
    )
```

```python
import functools

import jax
import jax.numpy as jnp
from jax import lax
from jax.experimental import pallas as pl
from jax.experimental.pallas import tpu as pltpu
from jax.sharding import PartitionSpec as P

MESH = pl.DeviceIdType.MESH
OWN, ACROSS_X, ACROSS_Y, DIAGONAL = range(4)
EARLY, LATE = range(2)


def shifted(block, axis, distance):
    devices = range(lax.axis_size(axis))
    route = [((i - distance) % len(devices), i) for i in devices]
    return lax.ppermute(block, axis, route)


def expert_apply(tokens_in, gate_mat, up_mat, down_mat):
    gate_part = jnp.dot(tokens_in, gate_mat, preferred_element_type=jnp.float32)
    upward = jnp.dot(tokens_in, up_mat, preferred_element_type=jnp.float32)
    hidden = (jax.nn.silu(gate_part) * upward).astype(jnp.bfloat16)
    return jnp.dot(hidden, down_mat, preferred_element_type=jnp.float32).astype(jnp.bfloat16)


def shards(incoming, expert_ids, gate_scores, gate_proj, up_proj, down_proj):
    arrived = shifted(incoming, "pp", 1)[0]
    tok_count, features = arrived.shape
    top_count = expert_ids.shape[2]
    expert_count = lax.axis_size("tp") * lax.axis_size("ep")
    capacity = min(tok_count, 2 * tok_count * top_count // expert_count)
    values = arrived.astype(jnp.float32)
    normed = (values * lax.rsqrt(jnp.mean(values * values, axis=1, keepdims=True) + 1e-06)).astype(
        jnp.bfloat16
    )
    chosen = expert_ids[0].reshape(-1)
    onehot = (chosen[:, None] == jnp.arange(expert_count, dtype=jnp.int32)[None, :]).astype(
        jnp.int32
    )
    before = jnp.cumsum(onehot, axis=0) - onehot
    slot_of = jnp.sum(before * onehot, axis=1)
    destination = chosen * capacity + slot_of
    owner_row = jnp.arange(chosen.shape[0], dtype=jnp.int32) // top_count
    source_row = (
        jnp.full((expert_count * capacity,), tok_count, jnp.int32).at[destination].set(owner_row)
    )
    occupied = jnp.zeros((expert_count * capacity,), jnp.int32).at[destination].set(1)
    with_blank = jnp.concatenate([normed, jnp.zeros((1, features), jnp.bfloat16)], axis=0)
    outgoing = with_blank[source_row].reshape(expert_count, capacity, features)
    occupied = occupied.reshape(expert_count, capacity)
    gate_mat, up_mat, down_mat = (gate_proj[0], up_proj[0], down_proj[0])
    received_rows = lax.all_to_all(outgoing, ("tp", "ep"), split_axis=0, concat_axis=0, tiled=True)
    flat_rows = received_rows.reshape(-1, features)
    flat_live = lax.all_to_all(
        occupied, ("tp", "ep"), split_axis=0, concat_axis=0, tiled=True
    ).reshape(-1)
    answered = expert_apply(flat_rows, gate_mat, up_mat, down_mat) * flat_live[:, None].astype(
        jnp.bfloat16
    )
    answered = answered.reshape(received_rows.shape)
    returned = lax.all_to_all(answered, ("tp", "ep"), split_axis=0, concat_axis=0, tiled=True)
    picked = returned.reshape(expert_count * capacity, features)[destination].reshape(
        tok_count, top_count, features
    )
    scores = gate_scores[0]
    weights = scores / jnp.sum(scores, axis=1, keepdims=True)
    combined = values + jnp.sum(weights[:, :, None] * picked.astype(jnp.float32), axis=1)
    return combined.astype(jnp.bfloat16)[None]


def exchange_kernel(
    sizes,
    incoming,
    ids_hbm,
    scores_hbm,
    gate_hbm,
    up_hbm,
    down_hbm,
    out_ref,
    gate_w,
    up_w,
    down_w,
    tok_early,
    tok_late,
    own_ids,
    own_scores,
    meta,
    hidden,
    kept_early,
    kept_late,
    passed_early,
    passed_late,
    partner_early,
    partner_late,
    to_early,
    to_late,
    from_early,
    from_late,
    via_early,
    via_late,
    done_early,
    lent_early,
    lent_late,
    sum_early,
    sum_late,
    send_sem,
    recv_sem,
    load_sem,
    hello,
):
    n_pp, n_tp, n_ep, top, chunks, pieces, lend = sizes
    features, ff = gate_w.shape
    pp, tp, ep = lax.axis_index("pp"), lax.axis_index("tp"), lax.axis_index("ep")
    other_core = tp + 1 - 2 * (tp % 2)
    at_x = {"ep": (ep + 1) % n_ep}
    at_y = {"tp": (tp + 2) % n_tp}
    at_core = {"tp": other_core}
    across = {"ep": (ep + 1) % n_ep, "tp": (tp + 2) % n_tp}
    far_x, far_y = {**at_x, **at_core}, {"tp": (other_core + 2) % n_tp}
    inner_core, outer_core = tp % 2 == 0, tp % 2 == 1
    ahead, behind = {"pp": (pp + 1) % n_pp}, {"pp": (pp + n_pp - 1) % n_pp}

    tok = (tok_early, tok_late)
    kept, passed = (kept_early, kept_late), (passed_early, passed_late)
    partner = (partner_early, partner_late)
    to, landed, via = (to_early, to_late), (from_early, from_late), (via_early, via_late)
    count = [t.shape[1] for t in tok]
    first_row = [count[LATE], 0]
    half = [n // 2 for n in count]
    lent, lent_sum = (lent_early, lent_late), (sum_early, sum_late)
    lent_rows = [h // p * m for h, p, m in zip(half, pieces, lend)]
    part = [[pl.ds(c * (n // chunks), n // chunks) for c in range(chunks)] for n in count]

    loads = []
    for src, dst in ((gate_hbm, gate_w), (up_hbm, up_w), (down_hbm, down_w)):
        loads.append(pltpu.make_async_copy(src.at[0], dst, load_sem.at[len(loads)]))
    own_rows = pltpu.make_async_copy(
        incoming.at[0, pl.ds(first_row[EARLY], count[EARLY])], tok_early.at[0], load_sem.at[3]
    )
    own_meta = [
        pltpu.make_async_copy(ids_hbm, own_ids, load_sem.at[4]),
        pltpu.make_async_copy(scores_hbm, own_scores, load_sem.at[5]),
    ]

    barrier = pltpu.get_barrier_semaphore()
    for peer in (at_x, at_y, at_core, behind):
        pl.semaphore_signal(barrier, inc=1, device_id=peer, device_id_type=MESH)
    for copy in own_meta:
        copy.start()
    own_rows.start()
    for copy in own_meta:
        copy.wait()

    def meta_slot(g, source):
        return 8 * g + source

    scores = own_scores[...]
    meta[meta_slot(LATE, 0), :top] = own_ids[...].astype(jnp.float32)
    meta[meta_slot(LATE, 0), top:] = scores / jnp.sum(scores, axis=0, keepdims=True)
    own_rows.wait()
    pl.semaphore_wait(barrier, 4)
    pl.semaphore_signal(hello, inc=1, device_id=ahead, device_id_type=MESH)

    lanes, sends = {}, {}

    def link(src, dst, peer, arrives, leaves):
        copy = pltpu.make_async_remote_copy(
            src_ref=src,
            dst_ref=dst,
            send_sem=send_sem.at[sends.setdefault(leaves, len(sends))],
            recv_sem=recv_sem.at[lanes.setdefault(arrives, len(lanes))],
            device_id=peer,
            device_id_type=MESH,
        )
        copy.start()

    def arrive(key, ref):
        sem = recv_sem.at[lanes[key]]
        pltpu.make_async_copy(ref, ref, sem).wait()

    def left(key, ref):
        sem = send_sem.at[sends[key]]
        pltpu.make_async_copy(ref, ref, sem).wait()

    def block(g, role, side, c):
        return tok[g].at[2 * role + side, part[g][c]]

    def share_x(g, c):
        link(block(g, OWN, 0, c), block(g, ACROSS_X, 0, c), at_x, (g, "plane", c), (g, "gather"))
        to_core(g, OWN, c)

    def share_y(g, c):
        link(block(g, OWN, 0, c), block(g, ACROSS_Y, 0, c), at_y, (g, "plane", c ^ 1), (g, "gather"))

    def share(g, c):
        share_x(g, c)
        if c % 2 == 1:
            share_y(g, c)
            share_y(g, c - 1)

    def to_core(g, role, c):
        link(block(g, role, 0, c), block(g, role, 1, c), at_core, (g, "core", role), (g, "gather"))

    def relay(g, c):
        arrive((g, "plane", c), tok[g].at[0, pl.ds(0, 2 * (count[g] // chunks))])
        for role, other, i in ((ACROSS_X, at_y, c), (ACROSS_Y, at_x, c ^ 1)):
            if c % 2 == 0:
                link(block(g, role, 0, i), block(g, DIAGONAL, 0, i), other, (g, "d"), (g, "gather"))
            to_core(g, role, i)

    def relay_diagonal(g):
        there, here = (tok[g].at[2 * DIAGONAL + side] for side in (1, 0))
        arrive((g, "d"), here)
        link(here, there, at_core, (g, "core", DIAGONAL), (g, "gather"))

    def meta_link(g, src, dst, peer, name):
        src, dst = meta_slot(g, src), meta_slot(g, dst)
        link(meta.at[src], meta.at[dst], peer, (g, "meta", name), "meta")

    def meta_arrive(g, name, n=1):
        arrive((g, "meta", name), meta.at[pl.ds(0, n)])

    def meta_first(g):
        meta_link(g, 0, 2, at_x, "plane")
        meta_link(g, 0, 4, at_y, "plane")
        meta_link(g, 0, 1, at_core, "near")

    def meta_second(g):
        if g == LATE:
            meta_link(g, 2, 6, at_y, "d")
        else:
            meta_arrive(g, "plane", 2)
        meta_link(g, 2, 3, at_core, "near")
        meta_link(g, 4, 5, at_core, "near")

    def meta_third(g):
        meta_arrive(g, "d")
        meta_link(g, 6, 7, at_core, "far" if g == EARLY else "near")

    mine = (tp * n_ep + ep).astype(jnp.float32)

    def weight(g, role):
        columns = []
        lane = lax.broadcasted_iota(jnp.int32, (count[g], meta.shape[2]), 1)
        row = lax.broadcasted_iota(jnp.int32, (count[g], meta.shape[2]), 0)
        for side in range(2):
            source = meta[meta_slot(g, 2 * role + side)]
            named = jnp.where(source[:top] == mine, source[top:], 0.0)
            named = jnp.sum(named, axis=0, keepdims=True)
            columns.append(
                jnp.sum(jnp.where(lane == row + first_row[g], named, 0.0), axis=1, keepdims=True)
            )
        return columns

    def expert(g, role):
        arrive((g, "core", role), tok[g].at[2 * role + 1])
        n = count[g]
        tokens_in = tok[g][2 * role : 2 * role + 2].reshape(2 * n, features)
        values = tokens_in.astype(jnp.float32)
        scale = lax.rsqrt(jnp.mean(values * values, axis=1, keepdims=True) + 1e-06)
        step = 256 if ff % 256 == 0 else 128
        for j in range(ff // step):
            cols = pl.ds(j * step, step)
            gate = jnp.dot(tokens_in, gate_w[:, cols], preferred_element_type=jnp.float32) * scale
            upward = jnp.dot(tokens_in, up_w[:, cols], preferred_element_type=jnp.float32) * scale
            hidden[: 2 * n, cols] = (gate / (1.0 + jnp.exp(-gate)) * upward).astype(jnp.bfloat16)
        inner = hidden[: 2 * n]
        here, there = weight(g, role)
        for j in range(features // 256):
            cols = pl.ds(j * 256, 256)
            y = jnp.dot(inner, down_w[:, cols], preferred_element_type=jnp.float32)
            y = y.astype(jnp.bfloat16).astype(jnp.float32)
            kept[g][role, :, cols] = (y[:n] * here).astype(jnp.bfloat16)
            passed[g][role, :, cols] = (y[n:] * there).astype(jnp.bfloat16)
        link(passed[g].at[role], partner[g].at[role], at_core, (g, "swap", role), (g, "return"))
        if role in (ACROSS_X, ACROSS_Y):
            k = (ACROSS_X, ACROSS_Y).index(role)

            @pl.when(inner_core)
            def _():
                rows = pl.ds(k * half[g], lent_rows[g])
                link(kept[g].at[role, rows], lent[g].at[k], at_core, (g, "lent"), (g, "lent"))

    def swapped(g, role):
        arrive((g, "swap", role), partner[g].at[role])

    def summed(g, role, lo, hi):
        return kept[g][role, lo:hi].astype(jnp.float32) + partner[g][role, lo:hi].astype(jnp.float32)

    def cuts(g):
        size = half[g] // pieces[g]
        return [(p * size, (p + 1) * size) for p in range(pieces[g])]

    def post(g, buffer, landing, lo, hi, value, peer, arrives, leaves="return"):
        to[g][buffer, lo:hi] = value.astype(jnp.bfloat16)
        rows = pl.ds(lo, hi - lo)
        link(to[g].at[buffer, rows], landing.at[rows], peer, (g, *arrives), (g, leaves))

    def send_diagonal(g):
        swapped(g, DIAGONAL)
        for p, (lo, hi) in enumerate(cuts(g)):
            value = summed(g, DIAGONAL, lo, hi)
            post(g, 2, via[g], lo, hi, value, at_x, ("across", p))
            lo, hi = lo + half[g], hi + half[g]
            value = summed(g, DIAGONAL, lo, hi)
            post(g, 2, via[g], lo, hi, value, at_y, ("across", p))

    def send_direct(g):
        swapped(g, ACROSS_X)
        swapped(g, ACROSS_Y)

        @pl.when(outer_core)
        def _():
            send_lent(g)
            for p in range(lend[g]):
                send_own(g, p, "outer")

        for p in range(lend[g], pieces[g]):
            send_own(g, p, "both")

    def send_own(g, p, leaves):
        for k, role, peer in ((0, ACROSS_X, at_x), (1, ACROSS_Y, at_y)):
            lo, hi = (edge + k * half[g] for edge in cuts(g)[p])
            value = summed(g, role, lo, hi)
            post(g, k, landed[g].at[k], lo, hi, value, peer, ("direct",), leaves)

    def send_lent(g):
        arrive((g, "lent"), via[g].at[pl.ds(0, 2 * lent_rows[g])])
        for k, role, peer in ((0, ACROSS_X, far_x), (1, ACROSS_Y, far_y)):
            for lo, hi in cuts(g)[: lend[g]]:
                rows = pl.ds(k * half[g] + lo, hi - lo)
                value = lent[g][k, lo:hi].astype(jnp.float32)
                value += passed[g][role, rows].astype(jnp.float32)
                lent_sum[g][k, lo:hi] = value.astype(jnp.bfloat16)
                source = lent_sum[g].at[k, pl.ds(lo, hi - lo)]
                link(source, landed[g].at[k, rows], peer, (g, "direct"), (g, "lent"))

    def send_merged(g, p):
        lo, hi = cuts(g)[p]
        arrive((g, "across", p), via[g].at[pl.ds(0, 2 * (hi - lo))])
        value = summed(g, ACROSS_Y, lo, hi) + via[g][lo:hi].astype(jnp.float32)
        post(g, 1, landed[g].at[1], lo, hi, value, at_y, ("merged", p))
        lo, hi = lo + half[g], hi + half[g]
        value = summed(g, ACROSS_X, lo, hi) + via[g][lo:hi].astype(jnp.float32)
        post(g, 0, landed[g].at[0], lo, hi, value, at_x, ("merged", p))

    def finish(g):
        swapped(g, OWN)
        arrive((g, "direct"), via[g])
        for p, span in enumerate(cuts(g)):
            arrive((g, "merged", p), via[g].at[pl.ds(0, 2 * (span[1] - span[0]))])
            for k in range(2):
                lo, hi = (edge + k * half[g] for edge in span)
                value = summed(g, OWN, lo, hi) + tok[g][0, lo:hi].astype(jnp.float32)
                value += landed[g][k, lo:hi].astype(jnp.float32)
                value += landed[g][1 - k, lo:hi].astype(jnp.float32)
                value = value.astype(jnp.bfloat16)
                if g == LATE:
                    out_ref[0, lo:hi] = value
                else:
                    done_early[lo:hi] = value
                    cut = pl.ds(lo + first_row[g], hi - lo)
                    link(done_early.at[pl.ds(lo, hi - lo)], out_ref.at[0, cut], ahead, "home", "home")

    def hopped(c):
        arrive(("hop", c), block(LATE, OWN, 0, c))
        share(LATE, c)

    meta_first(LATE)
    for c in range(chunks):
        link(incoming.at[0, part[LATE][c]], block(LATE, OWN, 0, c), ahead, ("hop", c), "hop")
    for c in range(chunks):
        share_x(EARLY, c)
        share_y(EARLY, c ^ 1)
        if c == chunks // 2:
            for copy in loads:
                copy.start()
            pl.semaphore_wait(hello, 1)
            meta_link_back = (meta.at[meta_slot(LATE, 0)], meta.at[meta_slot(EARLY, 0)])
            link(*meta_link_back, behind, (EARLY, "meta", "own"), "meta")
    meta_arrive(LATE, "plane", 2)
    meta_second(LATE)
    relay(EARLY, 0)
    relay(EARLY, 1)
    meta_arrive(EARLY, "own")
    meta_first(EARLY)
    meta_link(EARLY, 0, 6, across, "d")
    relay(EARLY, 2)
    hopped(0)
    hopped(1)
    relay(EARLY, 3)
    meta_second(EARLY)
    hopped(2)
    hopped(3)
    meta_third(LATE)
    for copy in loads:
        copy.wait()
    meta_arrive(EARLY, "near", 3)
    expert(EARLY, ACROSS_X)
    meta_third(EARLY)
    relay_diagonal(EARLY)
    expert(EARLY, ACROSS_Y)
    relay(LATE, 0)
    meta_arrive(EARLY, "far")
    expert(EARLY, DIAGONAL)
    relay(LATE, 1)
    relay(LATE, 2)
    send_diagonal(EARLY)
    send_direct(EARLY)
    relay(LATE, 3)
    expert(EARLY, OWN)
    meta_arrive(LATE, "near", 4)
    expert(LATE, ACROSS_X)
    relay_diagonal(LATE)
    expert(LATE, ACROSS_Y)
    for p in range(max(1, pieces[EARLY] // 2)):
        send_merged(EARLY, p)
    expert(LATE, DIAGONAL)
    for p in range(max(1, pieces[EARLY] // 2), pieces[EARLY]):
        send_merged(EARLY, p)
    send_diagonal(LATE)
    send_direct(LATE)
    finish(EARLY)
    expert(LATE, OWN)
    for p in range(pieces[LATE]):
        send_merged(LATE, p)
    finish(LATE)
    arrive("home", tok_early.at[0])
    left("hop", tok_late.at[0])
    left("home", tok_early.at[0])
    for g in (EARLY, LATE):
        left((g, "gather"), tok[g].at[pl.ds(0, 7)])
        left((g, "return"), tok[g].at[pl.ds(0, 6)])
        left((g, "lent"), via[g].at[pl.ds(0, 2 * lent_rows[g])])
        if lend[g] < pieces[g]:
            left((g, "both"), via[g].at[pl.ds(0, count[g] - 2 * lent_rows[g])])

    @pl.when(outer_core)
    def _():
        for g in (EARLY, LATE):
            left((g, "outer"), via[g].at[pl.ds(0, 2 * lent_rows[g])])

    left("meta", meta.at[pl.ds(0, 15)])


def fused(incoming, expert_ids, gate_scores, gate_proj, up_proj, down_proj):
    _, rows, features = incoming.shape
    top, ff = expert_ids.shape[2], gate_proj.shape[2]
    n_pp, n_tp, n_ep = (lax.axis_size(a) for a in ("pp", "tp", "ep"))
    early = rows // 2
    groups = (early, rows - early)
    chunks, pieces, lend = 4, (2, 2), (2, 1)
    hbm, vmem = pl.BlockSpec(memory_space=pl.ANY), pl.BlockSpec(memory_space=pltpu.VMEM)
    narrow = functools.partial(pltpu.VMEM, dtype=jnp.bfloat16)
    arrivals = 3 * chunks + 2 * (1 + 4 + 4 + 1 + sum(pieces)) + 3 + 8

    def pair(*lead):
        return [narrow((*lead, n, features)) for n in groups]

    return pl.pallas_call(
        functools.partial(exchange_kernel, (n_pp, n_tp, n_ep, top, chunks, pieces, lend)),
        out_shape=pltpu.VMEM(incoming.shape, incoming.dtype),
        in_specs=[hbm] * 6,
        out_specs=vmem,
        scratch_shapes=[
            narrow((features, ff)),
            narrow((features, ff)),
            narrow((ff, features)),
            *pair(8),
            pltpu.VMEM((top, rows), jnp.int32),
            pltpu.VMEM((top, rows), jnp.float32),
            pltpu.VMEM((16, 2 * top, rows), jnp.float32),
            narrow((2 * max(groups), ff)),
            *pair(4),
            *pair(4),
            *pair(4),
            *pair(3),
            *pair(2),
            *pair(),
            narrow((early, features)),
            *[narrow((2, n // 2 // p * m, features)) for n, p, m in zip(groups, pieces, lend)] * 2,
            pltpu.SemaphoreType.DMA((11 + sum(m < p for m, p in zip(lend, pieces)),)),
            pltpu.SemaphoreType.DMA((arrivals,)),
            pltpu.SemaphoreType.DMA((6,)),
            pltpu.SemaphoreType.REGULAR,
        ],
        compiler_params=pltpu.CompilerParams(collective_id=0, has_side_effects=True),
    )(incoming, expert_ids[0].T, gate_scores[0].T, gate_proj, up_proj, down_proj)


def solution(mesh):
    placed = (
        P("pp", ("tp", "ep"), None),
        P("pp", ("tp", "ep"), None),
        P("pp", ("tp", "ep"), None),
        P(("tp", "ep"), None, None),
        P(("tp", "ep"), None, None),
        P(("tp", "ep"), None, None),
    )
    square = mesh.shape["tp"] == 4 and mesh.shape["ep"] == 2 and mesh.shape["pp"] > 1
    return jax.shard_map(
        fused if square else shards,
        mesh=mesh,
        in_specs=placed,
        out_specs=P("pp", ("tp", "ep"), None),
        check_vma=False,
    )
```
